128 devices in a mesh: mp: 2 (over core), tile: 64 (over x, y, z).
Axes of the slice: x: 4, y: 4, z: 4, core: 2. Of those that a mesh axis runs over, the one named last changes fastest.
Arguments:
- state: float32 [2, 20, 256, 4096], P('mp', None, 'tile'), may hold values from -6 to 6
- guess: float32 [2, 24, 256, 4096], P('mp', None, 'tile'), may hold values from -6 to 6
- regrid: bfloat16 [2, 64, 64, 256, 256], P('mp', 'tile'), may hold values from -1 to 1
- regime: int32 [2, 256, 4096], P('mp', 'tile'), may hold values from 0 to 3
- land: int32 [2, 256, 4096], P('mp', 'tile'), may hold values 0 or 1
- land_temp: float32 [2, 256, 4096], P('mp', 'tile'), may hold values from -6 to 6
- exchange_rate: float32 [2, 4], P('mp'), may hold values from 0.05 to 0.3
- vertical: float32 [2, 19], P('mp'), may hold values from 0.05 to 0.3
- mixing: float32 [2], P('mp'), may hold values from 0.02 to 0.1
Outputs:
- final_state: float32 [2, 20, 256, 4096], P('mp', None, 'tile')
- forcing: float32 [2, 24, 256, 4096], P('mp', None, 'tile')
The draws below stay inside these ranges and needn't reach their ends.
All inputs are finite; a program needn't handle non-finite values. No bound on the sum of `land` on one device may be relied on, other than what follows from the above.
Results may differ from the reference program's by a relative error of at most 0.0029.
Values may be sent and summed in bfloat16 or wider, within the bound.
A program may use at most 128 MiB of HBM per device.

```python
import math
import jax
import jax.numpy as jnp
from jax import lax

LEV = 20
NT = 24
ITERS = 2
REGIMES = 4
FACE = 64
ROWS = 4
TILES = 64
COLS = 4096
GRID_ROWS = 256
SUB = 256


def draw_regrid(key, part):
    base = jax.random.fold_in(key, 7)
    first_key, second_key = jax.random.split(base)
    shape = (2, TILES, TILES, SUB, SUB)
    identity = jnp.eye(SUB, dtype=jnp.float32)
    spread = jax.random.normal(first_key, shape, jnp.float32) * (0.5 / math.sqrt(SUB))
    diagonal = jax.random.uniform(second_key, shape[:-1], jnp.float32, 0.45, 0.55)
    blocks = spread + diagonal[..., None] * identity
    return jnp.clip(blocks, -1.0, 1.0).astype(jnp.bfloat16)


def with_ends(values, stream_key, least, high):
    longest = values.shape.index(max(values.shape))
    spots = []
    for shift in (0, 1):
        where = [jax.random.randint(jax.random.fold_in(stream_key, axis), (), 0, length) for axis, length in enumerate(values.shape)]
        where[longest] = (where[longest] + shift) % values.shape[longest]
        spots.append(tuple(where))
    return values.at[spots[0]].set(least).at[spots[1]].set(high)


def block_scale(key, extent, cuts, low, largest):
    gain, own = 1.0, jax.random.fold_in(key, 6)
    for dim, blocks in cuts:
        draws = jnp.exp(jax.random.uniform(jax.random.fold_in(own, dim), (blocks,), jnp.float32, low / len(cuts), largest / len(cuts)))
        gain = gain * jnp.repeat(draws, extent[dim] // blocks).reshape([-1 if axis == dim else 1 for axis in range(len(extent))])
    return gain


def centred(own_key, dims, scale, limit, cuts=(), kind=jnp.bfloat16):
    drawn = jax.random.normal(own_key, dims, jnp.float32) * scale
    if len(cuts) > 0:
        drawn = block_scale(own_key, dims, cuts, -0.22, 0.18) * drawn
    return jnp.clip(drawn, min=-limit, max=limit).astype(kind)


def setup_inputs(seed: int = 0) -> dict:
    keys = jax.random.split(jax.random.key(seed), 10)
    state = centred(keys[0], (2, LEV, GRID_ROWS, COLS), 1.0, 6.0, ((0, 2), (2, 64)), jnp.float32)
    guess = centred(keys[1], (2, NT, GRID_ROWS, COLS), 1.0, 6.0, ((0, 2), (2, 64)), jnp.float32)
    regrid = draw_regrid(jax.random.fold_in(keys[9], 71), 0)
    regime = with_ends(jax.random.randint(keys[3], (2, GRID_ROWS, COLS), 0, REGIMES), jax.random.fold_in(keys[3], 1), 0, REGIMES - 1).astype(jnp.int32)
    land = with_ends((jax.random.randint(keys[4], (2, GRID_ROWS, COLS), 0, 10) < 3).astype(jnp.int32), jax.random.fold_in(keys[4], 1), 0, 1)
    land_temp = centred(keys[5], (2, GRID_ROWS, COLS), 1.0, 6.0, ((0, 2), (1, 64)), jnp.float32)
    exchange_rate = jnp.clip(jnp.exp(math.log(0.3) - 1.7917595 * jax.random.uniform(keys[6], (2, REGIMES), jnp.float32) ** block_scale(keys[6], (2, REGIMES), ((0, 2),), -0.2, 0.2)), 0.05, 0.3)
    vertical = jnp.clip(jnp.exp(math.log(0.3) - 1.7917595 * jax.random.uniform(keys[7], (2, LEV - 1), jnp.float32) ** block_scale(keys[7], (2, LEV - 1), ((0, 2),), -0.2, 0.2)), 0.05, 0.3)
    mixing = jnp.clip(jnp.exp(math.log(0.1) - 1.609438 * jax.random.uniform(keys[8], (2,), jnp.float32) ** block_scale(keys[8], (2,), ((0, 2),), -0.2, 0.2)), 0.02, 0.1)
    return dict(state=state, guess=guess, regrid=regrid, regime=regime, land=land, land_temp=land_temp, exchange_rate=exchange_rate, vertical=vertical, mixing=mixing)


def rate_field(regime, rates):
    field = jnp.zeros(regime.shape, jnp.float32)
    for kind_index in range(REGIMES):
        field = field + jnp.where(regime == kind_index, rates[kind_index], jnp.zeros((), jnp.float32))
    return field


def advance(column, force_now, coeff, land, land_temp, vertical, mixing):
    surface = column[0]
    boundary = jnp.where(land == 1, land_temp, force_now)
    flux = coeff * (boundary - surface)
    padded = jnp.pad(surface, ((1, 1), (0, 0)))
    lateral = padded[2:] + padded[:-2] + jnp.roll(surface, 1, axis=1) + jnp.roll(surface, -1, axis=1) - 4.0 * surface
    between = vertical[:, None, None] * (column[1:] - column[:-1])
    change = jnp.pad(between, ((0, 1), (0, 0), (0, 0))) - jnp.pad(between, ((1, 0), (0, 0), (0, 0)))
    updated = column + change
    updated = updated.at[0].add(flux + mixing * lateral)
    return updated


def run_window(column, forcing, coeff, land, land_temp, vertical, mixing):
    def one_step(carry, force_now):
        updated = advance(carry, force_now, coeff, land, land_temp, vertical, mixing)
        return updated, updated[0].astype(jnp.bfloat16)
    return lax.scan(one_step, column, forcing)


def regrid_trace(blocks, trace):
    pieces = trace.reshape(NT, TILES, ROWS, TILES, FACE).astype(jnp.float32)
    shaped = blocks.reshape(TILES, TILES, ROWS, FACE, ROWS, FACE).astype(jnp.float32)
    result = jnp.einsum('tarow,oapqrw->topaq', pieces, shaped, precision=lax.Precision.HIGHEST)
    return result.reshape(NT, GRID_ROWS, COLS)


def reference(state, guess, regrid, regime, land, land_temp, exchange_rate, vertical, mixing):
    coeffs = [rate_field(regime[member], exchange_rate[member]) for member in range(2)]
    forcing = guess
    finals = []
    for sweep_index in range(ITERS):
        finals = []
        traces = []
        for member in range(2):
            column, trace = run_window(state[member], forcing[member], coeffs[member], land[member], land_temp[member], vertical[member], mixing[member])
            finals.append(column)
            traces.append(trace)
        forcing = jnp.stack([regrid_trace(regrid[0], traces[1]), regrid_trace(regrid[1], traces[0])])
    return jnp.stack(finals), forcing
```

```python
import functools

import jax
import jax.numpy as jnp
from jax import lax
from jax.experimental import pallas as pl
from jax.experimental.pallas import tpu as pltpu
from jax.sharding import PartitionSpec as P

MESH = pl.DeviceIdType.MESH
F32 = jnp.float32
BF16 = jnp.bfloat16
K = 4
CHUNK = 8
ITERS = 2


def kernel(
    dims,
    state, guess, regrid, regime, land, land_temp, rates, vertical, mixing,
    final, forcing,
    us, force, wts, cx, raw, land_scale, land_add, own, hs, hr, q, sf, snd, rcv, gf,
    in_sem, coef_send, coef_recv, halo_send, halo_recv, trace_send, trace_recv, out_sem,
):
    tiles, levels, steps, size, regimes = dims
    macros = steps // K
    chunks = steps // CHUNK
    total = ITERS * macros
    last = ITERS * chunks - 1
    member = lax.axis_index("mp")
    tile = lax.axis_index("tile")
    has_up, has_down = tile > 0, tile < tiles - 1

    row = lax.broadcasted_iota(jnp.int32, (size, 128), 0)
    lane = lax.broadcasted_iota(jnp.int32, (size, 128), 1)
    strip_row = row % K

    small = [
        pltpu.make_async_copy(regime, raw.at[0], in_sem.at[0]),
        pltpu.make_async_copy(land, raw.at[1], in_sem.at[1]),
        pltpu.make_async_copy(land_temp, land_add, in_sem.at[2]),
    ]
    load_state = pltpu.make_async_copy(state, us.at[0], in_sem.at[3])
    load_guess = pltpu.make_async_copy(guess, force.at[pl.ds(0, steps)], in_sem.at[4])
    load_weights = pltpu.make_async_copy(regrid, wts, in_sem.at[5])
    for copy in small:
        copy.start()
    load_state.start()
    load_guess.start()
    load_weights.start()

    barrier = pltpu.get_barrier_semaphore()

    def greet(o, _):
        pl.semaphore_signal(barrier, inc=1, device_id=(1 - member, o), device_id_type=MESH)
        return 0

    lax.fori_loop(0, tiles, greet, 0)

    @pl.when(has_up)
    def _():
        pl.semaphore_signal(barrier, inc=1, device_id=(member, tile - 1), device_id_type=MESH)

    @pl.when(has_down)
    def _():
        pl.semaphore_signal(barrier, inc=1, device_id=(member, tile + 1), device_id_type=MESH)

    def clear(side):
        cx[2 * side] = jnp.zeros((size, 128), F32)

        def one(m, _):
            hr[m, side] = jnp.zeros((3, size, 128), BF16)
            return 0

        lax.fori_loop(0, total, one, 0)

    pl.when(jnp.logical_not(has_up))(lambda: clear(0))
    pl.when(jnp.logical_not(has_down))(lambda: clear(1))

    mix = mixing[0]
    mix_up = jnp.where(has_up, mix, 0.0)
    mix_down = jnp.where(has_down, mix, 0.0)
    vert = [vertical[0, l] for l in range(levels - 1)]

    for copy in small:
        copy.wait()
    kind = raw[0]
    coeff = jnp.zeros((size, 128), F32)
    for index in range(regimes):
        coeff = coeff + jnp.where(kind == index, rates[0, index], 0.0)
    is_land = raw[1] == 1
    cx[1] = coeff
    land_scale[...] = jnp.where(is_land, 0.0, coeff)
    land_add[...] = jnp.where(is_land, coeff * land_add[...], 0.0)

    def coef_copies():
        up = pltpu.make_async_remote_copy(
            cx.at[1], cx.at[2], coef_send.at[0], coef_recv.at[1], device_id=(member, tile - 1), device_id_type=MESH
        )
        down = pltpu.make_async_remote_copy(
            cx.at[1], cx.at[0], coef_send.at[1], coef_recv.at[0], device_id=(member, tile + 1), device_id_type=MESH
        )
        return up, down

    def halo_copies(m):
        up = pltpu.make_async_remote_copy(
            hs.at[m, pl.ds(0, 3)], hr.at[m, 1], halo_send.at[m, 0], halo_recv.at[m, 1],
            device_id=(member, tile - 1), device_id_type=MESH,
        )
        down = pltpu.make_async_remote_copy(
            hs.at[m, pl.ds(1, 3)], hr.at[m, 0], halo_send.at[m, 1], halo_recv.at[m, 0],
            device_id=(member, tile + 1), device_id_type=MESH,
        )
        return up, down

    def start(copies):
        up, down = copies
        pl.when(has_up)(lambda: up.start())
        pl.when(has_down)(lambda: down.start())

    def wait_recv(copies):
        up, down = copies
        pl.when(has_up)(lambda: down.wait_recv())
        pl.when(has_down)(lambda: up.wait_recv())

    def wait_send(copies):
        up, down = copies
        pl.when(has_up)(lambda: up.wait_send())
        pl.when(has_down)(lambda: down.wait_send())

    def advance(cols, count, c, source):
        between = [vert[l] * (cols[l + 1] - cols[l]) for l in range(min(count, levels - 1))]
        new = [cols[0] + between[0] + (source - c * cols[0])]
        for l in range(1, count):
            if l < levels - 1:
                new.append(cols[l] + between[l] - between[l - 1])
            else:
                new.append(cols[l] - between[l - 1])
        return new

    def responses(m, source, ahead):
        slot = m % 2
        srow = lax.broadcasted_iota(jnp.int32, (16, 128), 0) % K

        def one(p, _):
            rows = pl.ds(pl.multiple_of(p * 16, 16), 16)
            depth = 2 * K if ahead else K
            cols = [us[source, l, rows, :] for l in range(depth)]
            c = cx[1, rows, :]
            if ahead:
                for i in range(K):
                    cols = advance(cols, depth - 1 - i, c, q[i, rows, :])
            scale, add = land_scale[rows, :], land_add[rows, :]
            free = [cols[0]]
            for i in range(K - 1):
                cols = advance(cols, K - 1 - i, c, add + scale * force[K * m + i, rows, :])
                free.append(cols[0])
            for i in range(K):
                own[slot, i, rows, :] = free[i]
            hs[m, 0, rows, :] = jnp.where(srow == K - 1, pltpu.roll(free[3], 3, 0), free[1]).astype(BF16)
            hs[m, 1, rows, :] = free[0].astype(BF16)
            hs[m, 2, rows, :] = free[2].astype(BF16)
            hs[m, 3, rows, :] = jnp.where(srow == 0, pltpu.roll(free[3], 13, 0), free[1]).astype(BF16)
            return 0

        lax.fori_loop(0, size // 16, one, 0)

    def across(x):
        left = pltpu.roll(jnp.where(lane == 127, pltpu.roll(x, K, 0), x), 1, 1)
        right = pltpu.roll(jnp.where(lane == 0, pltpu.roll(x, size - K, 0), x), 127, 1)
        return left + right - 4.0 * x

    def simulate(m):
        slot = m % 2
        up_mid = hr[m, 0, 2].astype(F32)
        down_mid = hr[m, 1, 0].astype(F32)
        up_free = [hr[m, 0, 0].astype(F32), up_mid, hr[m, 0, 1].astype(F32), pltpu.roll(up_mid, 3, 0)]
        down_free = [hr[m, 1, 1].astype(F32), down_mid, hr[m, 1, 2].astype(F32), pltpu.roll(down_mid, size - 3, 0)]
        v0 = vert[0]
        gain = [1.0 - v0 - cx[k] for k in range(3)]
        mixes = (mix_up, mix, mix_down)
        up, mid, down = up_free[0], own[slot, 0], down_free[0]
        first = [None] * 3
        second = [None] * 3
        for i in range(K):
            above = jnp.where(strip_row == 0, pltpu.roll(up, size - 3, 0), pltpu.roll(mid, 1, 0))
            below = jnp.where(strip_row == K - 1, pltpu.roll(down, 3, 0), pltpu.roll(mid, size - 1, 0))
            sides = [None, mix * (above + below + across(mid)), None]
            q[i] = land_add[...] + land_scale[...] * force[K * m + i] + sides[1]
            if i == K - 1:
                break
            up_below = jnp.where(strip_row == K - 1, pltpu.roll(mid, 3, 0), pltpu.roll(up, size - 1, 0))
            down_above = jnp.where(strip_row == 0, pltpu.roll(mid, size - 3, 0), pltpu.roll(down, 1, 0))
            sides[0] = mix_up * (pltpu.roll(up, 1, 0) + up_below + across(up))
            sides[2] = mix_down * (pltpu.roll(down, size - 1, 0) + down_above + across(down))
            for k in range(3):
                response = sides[k]
                if first[k] is not None:
                    response = response + gain[k] * first[k]
                if second[k] is not None:
                    response = response + v0 * second[k]
                second[k] = None if first[k] is None else v0 * first[k]
                first[k] = response
            up = up_free[i + 1] + first[0]
            mid = own[slot, i + 1] + first[1]
            down = down_free[i + 1] + first[2]

    def swap(x):
        r = lax.broadcasted_iota(jnp.int32, x.shape, 0) % 2
        high = lax.broadcasted_iota(jnp.int32, x.shape, 1) >= 64
        other = pltpu.roll(x, 64, 1)
        n = x.shape[0]
        moved = jnp.where(r == 1, pltpu.roll(other, 1, 0), pltpu.roll(other, n - 1, 0))
        return jnp.where((r == 1) == high, x, moved)

    def columns(m, source):
        at = (m % 2) * K

        def one(p, _):
            rows = pl.ds(pl.multiple_of(p * 8, 8), 8)
            cols = [us[source, l, rows, :] for l in range(levels)]
            c = cx[1, rows, :]
            for i in range(K):
                cols = advance(cols, levels, c, q[i, rows, :])
                sf[pl.ds(p * 64 + at + i, 8, stride=8), :] = swap(cols[0])
            for l in range(levels):
                us[1, l, rows, :] = cols[l]
            return 0

        lax.fori_loop(0, size // 8, one, 0)

    def trace_copy(g, o):
        return pltpu.make_async_remote_copy(
            snd.at[g, o], rcv.at[g, tile], trace_send.at[g], trace_recv.at[g],
            device_id=(1 - member, o), device_id_type=MESH,
        )

    def whole_trace(g):
        return pltpu.make_async_remote_copy(
            snd.at[g], rcv.at[g], trace_send.at[g], trace_recv.at[g], device_id=(1 - member, tile), device_id_type=MESH
        )

    def send_trace(g):
        def pack(j, _):
            for h in range(2):
                low = sf[pl.ds(pl.multiple_of((j * 4 + h) * 8, 8), 8), :]
                high = sf[pl.ds(pl.multiple_of((j * 4 + 2 + h) * 8, 8), 8), :]
                snd[g, 2 * j + h] = jnp.concatenate([low, high], axis=0).astype(BF16)
            return 0

        lax.fori_loop(0, tiles // 2, pack, 0)

        def send(k, _):
            trace_copy(g, lax.rem(tile + k, tiles)).start()
            return 0

        lax.fori_loop(0, tiles, send, 0)

    def product(g, begin, count):
        def one(j, _):
            for h in range(2):
                a = 2 * j + h
                block = rcv[g, a]
                cells = jnp.concatenate([block[:8], block[8:]], axis=1)
                out = lax.dot_general(cells, wts[a], (((1,), (1,)), ((), ())), preferred_element_type=F32)
                gf[pl.ds(pl.multiple_of((j * 4 + h) * 8, 8), 8), :] = out[:, :128]
                gf[pl.ds(pl.multiple_of((j * 4 + 2 + h) * 8, 8), 8), :] = out[:, 128:]
            return 0

        lax.fori_loop(begin // 2, (begin + count) // 2, one, 0)

    def spread(g):
        def one(t, _):
            force[steps + g * CHUNK + t] = swap(gf[pl.ds(t, size, stride=8), :])
            return 0

        lax.fori_loop(0, CHUNK, one, 0)

    def put(g):
        part = g - (ITERS - 1) * chunks
        return pltpu.make_async_copy(
            force.at[pl.ds(steps + g * CHUNK, CHUNK)], forcing.at[pl.ds(part * CHUNK, CHUNK)], out_sem.at[part]
        )

    load_state.wait()
    load_guess.wait()
    responses(0, 0, False)
    pl.semaphore_wait(barrier, tiles + jnp.where(has_up, 1, 0) + jnp.where(has_down, 1, 0))
    start(coef_copies())
    start(halo_copies(0))
    wait_recv(coef_copies())

    def macro(m, _):
        within = lax.rem(m, macros)
        source = jnp.minimum(within, 1)
        odd = lax.rem(m, 2) == 1
        wait_recv(halo_copies(m))
        simulate(m)

        @pl.when(within < macros - 1)
        def _():
            responses(m + 1, source, True)
            start(halo_copies(m + 1))

        columns(m, source)

        @pl.when(odd)
        def _():
            send_trace(m // 2)

        @pl.when(m == 3)
        def _():
            load_weights.wait()

        @pl.when(jnp.logical_and(odd, m >= 3))
        def _():
            g = (m - 3) // 2
            whole_trace(g).wait_recv()
            product(g, 0, tiles // 2)

        @pl.when(jnp.logical_and(jnp.logical_not(odd), m >= 4))
        def _():
            g = (m - 4) // 2
            product(g, tiles // 2, tiles // 2)
            spread(g)

        @pl.when(m == 4)
        def _():
            responses(macros, 0, False)
            start(halo_copies(macros))

        return 0

    lax.fori_loop(0, total, macro, 0)

    put_final = pltpu.make_async_copy(us.at[1], final, out_sem.at[chunks])
    put_final.start()
    put(last - 2).start()
    product(last - 1, tiles // 2, tiles // 2)
    spread(last - 1)
    put(last - 1).start()
    whole_trace(last).wait_recv()
    product(last, 0, tiles)
    spread(last)
    put(last).start()

    wait_send(coef_copies())

    def drain(m, _):
        wait_send(halo_copies(m))
        return 0

    lax.fori_loop(0, total, drain, 0)

    def drain_trace(g, _):
        whole_trace(g).wait_send()
        return 0

    lax.fori_loop(0, last + 1, drain_trace, 0)
    put_final.wait()
    for g in range(last - 2, last + 1):
        put(g).wait()


def to_tiles(x):
    n, rows, width = x.shape
    return x.reshape(n, rows, width // 128, 128).transpose(0, 2, 1, 3).reshape(n, rows * width // 128, 128)


def from_tiles(x, rows):
    n, size, _ = x.shape
    return x.reshape(n, size // rows, rows, 128).transpose(0, 2, 1, 3).reshape(n, rows, size // rows * 128)


def on_device(state, guess, regrid, regime, land, land_temp, exchange_rate, vertical, mixing):
    levels, rows, width = state.shape[1:]
    steps = guess.shape[1]
    tiles = lax.axis_size("tile")
    size = rows * width // 128
    cells = regrid.shape[-1]
    macros = ITERS * steps // K
    groups = ITERS * steps // CHUNK
    dims = (tiles, levels, steps, size, exchange_rate.shape[1])
    hbm = pl.BlockSpec(memory_space=pl.ANY)
    smem = pl.BlockSpec(memory_space=pltpu.SMEM)
    dma = pltpu.SemaphoreType.DMA
    final, forcing = pl.pallas_call(
        functools.partial(kernel, dims),
        out_shape=(
            jax.ShapeDtypeStruct((levels, size, 128), F32),
            jax.ShapeDtypeStruct((steps, size, 128), F32),
        ),
        in_specs=[hbm] * 6 + [smem] * 3,
        out_specs=(hbm, hbm),
        scratch_shapes=[
            pltpu.VMEM((2, levels, size, 128), F32),
            pltpu.VMEM(((ITERS + 1) * steps, size, 128), F32),
            pltpu.VMEM((tiles, cells, cells), BF16),
            pltpu.VMEM((3, size, 128), F32),
            pltpu.VMEM((2, size, 128), jnp.int32),
            pltpu.VMEM((size, 128), F32),
            pltpu.VMEM((size, 128), F32),
            pltpu.VMEM((2, K, size, 128), F32),
            pltpu.VMEM((macros, 4, size, 128), BF16),
            pltpu.VMEM((macros, 2, 3, size, 128), BF16),
            pltpu.VMEM((K, size, 128), F32),
            pltpu.VMEM((8 * size, 128), F32),
            pltpu.VMEM((groups, tiles, 16, 128), BF16),
            pltpu.VMEM((groups, tiles, 16, 128), BF16),
            pltpu.VMEM((8 * size, 128), F32),
            dma((6,)),
            dma((2,)),
            dma((2,)),
            dma((macros, 2)),
            dma((macros, 2)),
            dma((groups,)),
            dma((groups,)),
            dma((groups // ITERS + 1,)),
        ],
        compiler_params=pltpu.CompilerParams(
            collective_id=0, has_side_effects=True, vmem_limit_bytes=60 * 1024 * 1024
        ),
    )(
        to_tiles(state[0]),
        to_tiles(guess[0]),
        regrid[0, 0],
        to_tiles(regime)[0],
        to_tiles(land)[0],
        to_tiles(land_temp)[0],
        exchange_rate,
        vertical,
        mixing,
    )
    return from_tiles(final, rows)[None], from_tiles(forcing, rows)[None]


def solution(mesh):
    return jax.shard_map(
        on_device,
        mesh=mesh,
        in_specs=(
            P("mp", None, "tile", None),
            P("mp", None, "tile", None),
            P("mp", "tile", None, None, None),
            P("mp", "tile", None),
            P("mp", "tile", None),
            P("mp", "tile", None),
            P("mp", None),
            P("mp", None),
            P("mp"),
        ),
        out_specs=(P("mp", None, "tile", None), P("mp", None, "tile", None)),
        check_vma=False,
    )
```

```python
import functools

import jax
import jax.numpy as jnp
from jax import lax
from jax.experimental import pallas as pl
from jax.experimental.pallas import tpu as pltpu
from jax.sharding import PartitionSpec as P

MESH = pl.DeviceIdType.MESH
F32 = jnp.float32
BF16 = jnp.bfloat16
K = 4
CHUNK = 8
ITERS = 2
UNROLL = 4


def kernel(
    dims,
    state, guess, regrid, regime, land, land_temp, rates, vertical, mixing,
    final, forcing,
    us, force, wts, cx, raw, land_scale, land_add, own, hs0, hs1, hs2, hr0, hr1, hr2, q, tr, sf, snd, rcv, gf,
    in_sem, coef_send, coef_recv, halo_send, halo_recv, trace_send, trace_recv, out_sem,
):
    tiles, levels, steps, size, regimes = dims
    macros = steps // K
    chunks = steps // CHUNK
    total = ITERS * macros
    last = ITERS * chunks - 1
    member = lax.axis_index("mp")
    tile = lax.axis_index("tile")
    has_up, has_down = tile > 0, tile < tiles - 1

    row = lax.broadcasted_iota(jnp.int32, (size, 128), 0)
    lane = lax.broadcasted_iota(jnp.int32, (size, 128), 1)
    strip_row = row % K

    small = [
        pltpu.make_async_copy(regime, raw.at[0], in_sem.at[0]),
        pltpu.make_async_copy(land, raw.at[1], in_sem.at[1]),
        pltpu.make_async_copy(land_temp, land_add, in_sem.at[2]),
    ]
    def load_state(begin, count, sem):
        part = pl.ds(begin, count)
        return pltpu.make_async_copy(state.at[part], us.at[0, part], in_sem.at[sem])

    def load_guess(begin, count, sem):
        part = pl.ds(begin, count)
        return pltpu.make_async_copy(guess.at[part], force.at[part], in_sem.at[sem])

    early = [load_state(0, K, 3), load_guess(0, K, 4)]
    late = [load_state(K, levels - K, 5), load_guess(K, steps - K, 6)]
    load_weights = pltpu.make_async_copy(regrid, wts, in_sem.at[7])
    for copy in small + early + late:
        copy.start()

    barrier = pltpu.get_barrier_semaphore()

    def greet(o, _):
        pl.semaphore_signal(barrier, inc=1, device_id=(1 - member, o), device_id_type=MESH)
        return 0

    lax.fori_loop(0, tiles, greet, 0)

    @pl.when(has_up)
    def _():
        pl.semaphore_signal(barrier, inc=1, device_id=(member, tile - 1), device_id_type=MESH)

    @pl.when(has_down)
    def _():
        pl.semaphore_signal(barrier, inc=1, device_id=(member, tile + 1), device_id_type=MESH)

    def clear(side):
        cx[2 * side] = jnp.zeros((size, 128), F32)

        def one(m, _):
            hr0[m, side] = jnp.zeros((size, 128), BF16)
            hr1[m, side] = jnp.zeros((size, 128), BF16)
            hr2[m, side] = jnp.zeros((size // 2, 128), BF16)
            return 0

        lax.fori_loop(0, total, one, 0)

    pl.when(jnp.logical_not(has_up))(lambda: clear(0))
    pl.when(jnp.logical_not(has_down))(lambda: clear(1))

    mix = mixing[0]
    mix_up = jnp.where(has_up, mix, 0.0)
    mix_down = jnp.where(has_down, mix, 0.0)
    vert = [vertical[0, l] for l in range(levels - 1)]

    for copy in small:
        copy.wait()
    kind = raw[0]
    coeff = jnp.zeros((size, 128), F32)
    for index in range(regimes):
        coeff = coeff + jnp.where(kind == index, rates[0, index], 0.0)
    is_land = raw[1] == 1
    cx[1] = coeff
    land_scale[...] = jnp.where(is_land, 0.0, coeff)
    land_add[...] = jnp.where(is_land, coeff * land_add[...], 0.0)

    def coef_copies():
        up = pltpu.make_async_remote_copy(
            cx.at[1], cx.at[2], coef_send.at[0], coef_recv.at[1], device_id=(member, tile - 1), device_id_type=MESH
        )
        down = pltpu.make_async_remote_copy(
            cx.at[1], cx.at[0], coef_send.at[1], coef_recv.at[0], device_id=(member, tile + 1), device_id_type=MESH
        )
        return up, down

    def halo_copies(m, part):
        sources = (hs0.at[m], hs0.at[m]), (hs1.at[m, 0], hs1.at[m, 1]), (hs2.at[m, 0], hs2.at[m, 1])
        target = (hr0, hr1, hr2)[part]
        up = pltpu.make_async_remote_copy(
            sources[part][0], target.at[m, 1], halo_send.at[m, part, 0], halo_recv.at[m, part, 1],
            device_id=(member, tile - 1), device_id_type=MESH,
        )
        down = pltpu.make_async_remote_copy(
            sources[part][1], target.at[m, 0], halo_send.at[m, part, 1], halo_recv.at[m, part, 0],
            device_id=(member, tile + 1), device_id_type=MESH,
        )
        return up, down

    def start(copies):
        up, down = copies
        pl.when(has_up)(lambda: up.start())
        pl.when(has_down)(lambda: down.start())

    def wait_recv(copies):
        up, down = copies
        pl.when(has_up)(lambda: down.wait_recv())
        pl.when(has_down)(lambda: up.wait_recv())

    def wait_send(copies):
        up, down = copies
        pl.when(has_up)(lambda: up.wait_send())
        pl.when(has_down)(lambda: down.wait_send())

    def advance(cols, count, c, source):
        between = [vert[l] * (cols[l + 1] - cols[l]) for l in range(min(count, levels - 1))]
        new = [cols[0] + between[0] + (source - c * cols[0])]
        for l in range(1, count):
            if l < levels - 1:
                new.append(cols[l] + between[l] - between[l - 1])
            else:
                new.append(cols[l] - between[l - 1])
        return new

    def responses(m, source, ahead):
        slot = m % 2
        srow = lax.broadcasted_iota(jnp.int32, (16, 128), 0) % K

        def one(p, _):
            rows = pl.ds(pl.multiple_of(p * 16, 16), 16)
            depth = 2 * K if ahead else K
            cols = [us[source, l, rows, :] for l in range(depth)]
            c = cx[1, rows, :]
            if ahead:
                for i in range(K):
                    cols = advance(cols, depth - 1 - i, c, q[i, rows, :])
            scale, add = land_scale[rows, :], land_add[rows, :]
            free = [cols[0]]
            for i in range(K - 1):
                cols = advance(cols, K - 1 - i, c, add + scale * force[K * m + i, rows, :])
                free.append(cols[0])
            for i in range(K):
                own[slot, i, rows, :] = free[i]
            hs0[m, rows, :] = free[0].astype(BF16)
            hs1[m, 0, rows, :] = jnp.where(srow == K - 1, pltpu.roll(free[3], 3, 0), free[1]).astype(BF16)
            hs1[m, 1, rows, :] = jnp.where(srow == 0, pltpu.roll(free[3], 13, 0), free[1]).astype(BF16)
            return 0

        lax.fori_loop(0, size // 16, one, 0)
        start(halo_copies(m, 0))
        start(halo_copies(m, 1))
        half = size // 2
        near, far = own[slot, 2, :half, :], own[slot, 2, half:, :]
        upper = strip_row[:half] < 2
        hs2[m, 0] = jnp.where(upper, near, pltpu.roll(far, 2, 0)).astype(BF16)
        hs2[m, 1] = jnp.where(upper, pltpu.roll(far, half - 2, 0), near).astype(BF16)
        start(halo_copies(m, 2))

    def across(x):
        left = pltpu.roll(jnp.where(lane == 127, pltpu.roll(x, K, 0), x), 1, 1)
        right = pltpu.roll(jnp.where(lane == 0, pltpu.roll(x, size - K, 0), x), 127, 1)
        return left + right - 4.0 * x

    def simulate(m):
        slot = m % 2
        v0 = vert[0]

        def source(i, lateral):
            q[i] = land_add[...] + land_scale[...] * force[K * m + i] + mix * lateral

        def shifted(mid):
            return pltpu.roll(mid, size - 3, 0), pltpu.roll(mid, 3, 0)

        top, bottom = strip_row == 0, strip_row == K - 1
        wait_recv(halo_copies(m, 0))
        up, mid, down = hr0[m, 0].astype(F32), own[slot, 0], hr0[m, 1].astype(F32)
        last_mid, first_mid = shifted(mid)
        above = jnp.where(top, pltpu.roll(up, size - 3, 0), pltpu.roll(mid, 1, 0))
        below = jnp.where(bottom, pltpu.roll(down, 3, 0), pltpu.roll(mid, size - 1, 0))
        lateral = above + below + across(mid)
        source(0, lateral)
        mid_w = mix * lateral
        below = jnp.where(bottom, first_mid, pltpu.roll(up, size - 1, 0))
        up_w = mix_up * (pltpu.roll(up, 1, 0) + below + across(up))
        above = jnp.where(top, last_mid, pltpu.roll(down, 1, 0))
        down_w = mix_down * (above + pltpu.roll(down, size - 1, 0) + across(down))
        wait_recv(halo_copies(m, 1))
        from_up = strip_row >= 2
        up_free, down_free = hr1[m, 0].astype(F32), hr1[m, 1].astype(F32)
        up, mid, down = up_free + up_w, own[slot, 1] + mid_w, down_free + down_w
        edge_mix = jnp.where(from_up, mix_up, mix_down)
        edge_gain = 1.0 - v0 - jnp.where(from_up, cx[0], cx[2])
        mid_gain = 1.0 - v0 - cx[1]
        edge = jnp.where(from_up, up, down)
        edge_w = jnp.where(from_up, up_w, down_w)
        last_mid, first_mid = shifted(mid)
        above = jnp.where(top, pltpu.roll(up, size - 3, 0), pltpu.roll(mid, 1, 0))
        below = jnp.where(bottom, pltpu.roll(down, 3, 0), pltpu.roll(mid, size - 1, 0))
        lateral = above + below + across(mid)
        source(1, lateral)
        mid_next = mid_gain * mid_w + mix * lateral
        above = jnp.where(top, last_mid, pltpu.roll(jnp.where(top, down, up), 1, 0))
        below = jnp.where(bottom, first_mid, pltpu.roll(jnp.where(bottom, up, down), size - 1, 0))
        edge_next = edge_gain * edge_w + edge_mix * (above + below + across(edge))
        wait_recv(halo_copies(m, 2))
        half = size // 2
        up_free2, down_free2 = hr2[m, 0].astype(F32), hr2[m, 1].astype(F32)
        low = from_up[:half]
        free = jnp.concatenate(
            [
                jnp.where(low, up_free2, down_free2),
                jnp.where(low, pltpu.roll(up_free2, 2, 0), pltpu.roll(down_free2, half - 2, 0)),
            ],
            axis=0,
        )
        mid, edge = own[slot, 2] + mid_next, free + edge_next
        last_mid, first_mid = shifted(mid)

        def middle(mid, edge):
            above = jnp.where(top, pltpu.roll(edge, size - 3, 0), pltpu.roll(mid, 1, 0))
            below = jnp.where(bottom, pltpu.roll(edge, 3, 0), pltpu.roll(mid, size - 1, 0))
            return above + below + across(mid)

        lateral = middle(mid, edge)
        source(2, lateral)
        mid_w = mid_gain * mid_next + v0 * v0 * mid_w + mix * lateral
        above = jnp.where(top, last_mid, pltpu.roll(edge, 1, 0))
        below = jnp.where(bottom, first_mid, pltpu.roll(edge, size - 1, 0))
        edge_w = edge_gain * edge_next + v0 * v0 * edge_w + edge_mix * (above + below + across(edge))
        free = jnp.where(from_up, pltpu.roll(up_free, 3, 0), pltpu.roll(down_free, size - 3, 0))
        source(3, middle(own[slot, 3] + mid_w, free + edge_w))

    def swap(x):
        r = lax.broadcasted_iota(jnp.int32, x.shape, 0) % 2
        high = lax.broadcasted_iota(jnp.int32, x.shape, 1) >= 64
        other = pltpu.roll(x, 64, 1)
        n = x.shape[0]
        moved = jnp.where(r == 1, pltpu.roll(other, 1, 0), pltpu.roll(other, n - 1, 0))
        return jnp.where((r == 1) == high, x, moved)

    def columns(m, source):
        at = (m % 2) * K

        def one(p, _):
            rows = pl.ds(pl.multiple_of(p * 8, 8), 8)
            cols = [us[source, l, rows, :] for l in range(levels)]
            c = cx[1, rows, :]
            for i in range(K):
                cols = advance(cols, levels, c, q[i, rows, :])
                tr[i, rows, :] = cols[0]
            for l in range(levels):
                us[1, l, rows, :] = cols[l]
            return 0

        lax.fori_loop(0, size // 8, one, 0)
        for i in range(K):
            sf[pl.ds(at + i, size, stride=8), :] = swap(tr[i])

    def trace_copy(g, o):
        return pltpu.make_async_remote_copy(
            snd.at[g, o], rcv.at[g, tile], trace_send.at[g], trace_recv.at[g],
            device_id=(1 - member, o), device_id_type=MESH,
        )

    def whole_trace(g):
        return pltpu.make_async_remote_copy(
            snd.at[g], rcv.at[g], trace_send.at[g], trace_recv.at[g], device_id=(1 - member, tile), device_id_type=MESH
        )

    def pack_trace(g):
        def pack(j, _):
            for h in range(2):
                low = sf[pl.ds(pl.multiple_of((j * 4 + h) * 8, 8), 8), :]
                high = sf[pl.ds(pl.multiple_of((j * 4 + 2 + h) * 8, 8), 8), :]
                snd[g, 2 * j + h] = jnp.concatenate([low, high], axis=0).astype(BF16)
            return 0

        lax.fori_loop(0, tiles // 2, pack, 0, unroll=4)

    def send_trace(g, begin, end):
        def send(k, _):
            trace_copy(g, lax.rem(tile + k, tiles)).start()
            return 0

        lax.fori_loop(begin, end, send, 0)

    def product(g, begin, count):
        def one(j, _):
            for h in range(2):
                a = 2 * j + h
                block = rcv[g, a]
                cells = jnp.concatenate([block[:8], block[8:]], axis=1)
                out = lax.dot_general(cells, wts[a], (((1,), (1,)), ((), ())), preferred_element_type=F32)
                gf[pl.ds(pl.multiple_of((j * 4 + h) * 8, 8), 8), :] = out[:, :128]
                gf[pl.ds(pl.multiple_of((j * 4 + 2 + h) * 8, 8), 8), :] = out[:, 128:]
            return 0

        lax.fori_loop(begin // 2, (begin + count) // 2, one, 0, unroll=UNROLL)

    def spread(g):
        def one(t, _):
            force[steps + g * CHUNK + t] = swap(gf[pl.ds(t, size, stride=8), :])
            return 0

        lax.fori_loop(0, CHUNK, one, 0)

    def put(g):
        part = g - (ITERS - 1) * chunks
        return pltpu.make_async_copy(
            force.at[pl.ds(steps + g * CHUNK, CHUNK)], forcing.at[pl.ds(part * CHUNK, CHUNK)], out_sem.at[part]
        )

    for copy in early:
        copy.wait()
    pl.semaphore_wait(barrier, tiles + jnp.where(has_up, 1, 0) + jnp.where(has_down, 1, 0))
    responses(0, 0, False)
    start(coef_copies())
    for copy in late:
        copy.wait()
    load_weights.start()
    wait_recv(coef_copies())

    def macro(m, _):
        within = lax.rem(m, macros)
        source = jnp.minimum(within, 1)
        odd = lax.rem(m, 2) == 1
        simulate(m)

        @pl.when(within < macros - 1)
        def _():
            responses(m + 1, source, True)

        @pl.when(jnp.logical_and(jnp.logical_not(odd), m >= 2))
        def _():
            send_trace(m // 2 - 1, tiles // 2, tiles)

        columns(m, source)

        @pl.when(odd)
        def _():
            pack_trace(m // 2)
            send_trace(m // 2, 0, jnp.where(m == total - 1, tiles, tiles // 2))

        @pl.when(m == 3)
        def _():
            load_weights.wait()

        @pl.when(jnp.logical_and(odd, m >= 3))
        def _():
            g = (m - 3) // 2
            whole_trace(g).wait_recv()
            product(g, 0, tiles // 2)

        @pl.when(jnp.logical_and(jnp.logical_not(odd), m >= 4))
        def _():
            g = (m - 4) // 2
            product(g, tiles // 2, tiles // 2)
            spread(g)

        @pl.when(m == 4)
        def _():
            responses(macros, 0, False)

        return 0

    lax.fori_loop(0, total, macro, 0)

    put_final = pltpu.make_async_copy(us.at[1], final, out_sem.at[chunks])
    put_final.start()
    put(last - 2).start()
    product(last - 1, tiles // 2, tiles // 2)
    spread(last - 1)
    put(last - 1).start()
    whole_trace(last).wait_recv()
    product(last, 0, tiles)
    spread(last)
    put(last).start()

    wait_send(coef_copies())

    def drain(m, _):
        for part in range(3):
            wait_send(halo_copies(m, part))
        return 0

    lax.fori_loop(0, total, drain, 0)

    def drain_trace(g, _):
        whole_trace(g).wait_send()
        return 0

    lax.fori_loop(0, last + 1, drain_trace, 0)
    put_final.wait()
    for g in range(last - 2, last + 1):
        put(g).wait()


def to_tiles(x):
    n, rows, width = x.shape
    return x.reshape(n, rows, width // 128, 128).transpose(0, 2, 1, 3).reshape(n, rows * width // 128, 128)


def from_tiles(x, rows):
    n, size, _ = x.shape
    return x.reshape(n, size // rows, rows, 128).transpose(0, 2, 1, 3).reshape(n, rows, size // rows * 128)


def on_device(state, guess, regrid, regime, land, land_temp, exchange_rate, vertical, mixing):
    levels, rows, width = state.shape[1:]
    steps = guess.shape[1]
    tiles = lax.axis_size("tile")
    size = rows * width // 128
    cells = regrid.shape[-1]
    macros = ITERS * steps // K
    groups = ITERS * steps // CHUNK
    dims = (tiles, levels, steps, size, exchange_rate.shape[1])
    hbm = pl.BlockSpec(memory_space=pl.ANY)
    smem = pl.BlockSpec(memory_space=pltpu.SMEM)
    dma = pltpu.SemaphoreType.DMA
    final, forcing = pl.pallas_call(
        functools.partial(kernel, dims),
        out_shape=(
            jax.ShapeDtypeStruct((levels, size, 128), F32),
            jax.ShapeDtypeStruct((steps, size, 128), F32),
        ),
        in_specs=[hbm] * 6 + [smem] * 3,
        out_specs=(hbm, hbm),
        scratch_shapes=[
            pltpu.VMEM((2, levels, size, 128), F32),
            pltpu.VMEM(((ITERS + 1) * steps, size, 128), F32),
            pltpu.VMEM((tiles, cells, cells), BF16),
            pltpu.VMEM((3, size, 128), F32),
            pltpu.VMEM((2, size, 128), jnp.int32),
            pltpu.VMEM((size, 128), F32),
            pltpu.VMEM((size, 128), F32),
            pltpu.VMEM((2, K, size, 128), F32),
            pltpu.VMEM((macros, size, 128), BF16),
            pltpu.VMEM((macros, 2, size, 128), BF16),
            pltpu.VMEM((macros, 2, size // 2, 128), BF16),
            pltpu.VMEM((macros, 2, size, 128), BF16),
            pltpu.VMEM((macros, 2, size, 128), BF16),
            pltpu.VMEM((macros, 2, size // 2, 128), BF16),
            pltpu.VMEM((K, size, 128), F32),
            pltpu.VMEM((K, size, 128), F32),
            pltpu.VMEM((8 * size, 128), F32),
            pltpu.VMEM((groups, tiles, 16, 128), BF16),
            pltpu.VMEM((groups, tiles, 16, 128), BF16),
            pltpu.VMEM((8 * size, 128), F32),
            dma((8,)),
            dma((2,)),
            dma((2,)),
            dma((macros, 3, 2)),
            dma((macros, 3, 2)),
            dma((groups,)),
            dma((groups,)),
            dma((groups // ITERS + 1,)),
        ],
        compiler_params=pltpu.CompilerParams(
            collective_id=0, has_side_effects=True, vmem_limit_bytes=60 * 1024 * 1024
        ),
    )(
        to_tiles(state[0]),
        to_tiles(guess[0]),
        regrid[0, 0],
        to_tiles(regime)[0],
        to_tiles(land)[0],
        to_tiles(land_temp)[0],
        exchange_rate,
        vertical,
        mixing,
    )
    return from_tiles(final, rows)[None], from_tiles(forcing, rows)[None]


def solution(mesh):
    return jax.shard_map(
        on_device,
        mesh=mesh,
        in_specs=(
            P("mp", None, "tile", None),
            P("mp", None, "tile", None),
            P("mp", "tile", None, None, None),
            P("mp", "tile", None),
            P("mp", "tile", None),
            P("mp", "tile", None),
            P("mp", None),
            P("mp", None),
            P("mp"),
        ),
        out_specs=(P("mp", None, "tile", None), P("mp", None, "tile", None)),
        check_vma=False,
    )
```

```python
import functools

import jax
import jax.numpy as jnp
from jax import lax
from jax.experimental import pallas as pl
from jax.experimental.pallas import tpu as pltpu
from jax.sharding import PartitionSpec as P

MESH = pl.DeviceIdType.MESH
F32 = jnp.float32
BF16 = jnp.bfloat16
K = 4
CHUNK = 8
ITERS = 2
UNROLL = 4
LAG = 4


def kernel(
    dims,
    state, guess, regrid, regime, land, land_temp, rates_in, vertical_in, mixing,
    final, forcing,
    rates, vertical, us, force, wts, cx, raw, land_scale, land_add, own, hs, hr, q, tr, sf, snd, rcv, gf,
    in_sem, coef_send, coef_recv, halo_send, halo_recv, trace_send, trace_recv, out_sem,
):
    tiles, levels, steps, size, regimes = dims
    macros = steps // K
    chunks = steps // CHUNK
    total = ITERS * macros
    slots = macros + LAG * (ITERS - 1)
    last = ITERS * chunks - 1
    member = lax.axis_index("mp")
    tile = lax.axis_index("tile")
    has_up, has_down = tile > 0, tile < tiles - 1

    row = lax.broadcasted_iota(jnp.int32, (size, 128), 0)
    lane = lax.broadcasted_iota(jnp.int32, (size, 128), 1)
    strip_row = row % K

    small = [
        pltpu.make_async_copy(regime, raw.at[0], in_sem.at[0]),
        pltpu.make_async_copy(land, raw.at[1], in_sem.at[1]),
        pltpu.make_async_copy(land_temp, land_add, in_sem.at[2]),
        pltpu.make_async_copy(rates_in, rates, in_sem.at[8]),
        pltpu.make_async_copy(vertical_in, vertical, in_sem.at[9]),
    ]
    def load_state(begin, count, sem):
        part = pl.ds(begin, count)
        return pltpu.make_async_copy(state.at[part], us.at[0, part], in_sem.at[sem])

    def load_guess(begin, count, sem):
        part = pl.ds(begin, count)
        return pltpu.make_async_copy(guess.at[part], force.at[part], in_sem.at[sem])

    early = [load_state(0, K, 3), load_guess(0, K, 4)]
    late = [load_state(K, levels - K, 5), load_guess(K, steps - K, 6)]
    load_weights = pltpu.make_async_copy(regrid, wts, in_sem.at[7])
    for copy in small + early + late:
        copy.start()

    barrier = pltpu.get_barrier_semaphore()

    def greet(o, _):
        pl.semaphore_signal(barrier, inc=1, device_id=(1 - member, o), device_id_type=MESH)
        return 0

    lax.fori_loop(0, tiles, greet, 0, unroll=4)

    @pl.when(has_up)
    def _():
        pl.semaphore_signal(barrier, inc=1, device_id=(member, tile - 1), device_id_type=MESH)

    @pl.when(has_down)
    def _():
        pl.semaphore_signal(barrier, inc=1, device_id=(member, tile + 1), device_id_type=MESH)

    def clear(side):
        cx[2 * side] = jnp.zeros((size, 128), F32)

        def one(m, _):
            hr[m, side] = jnp.zeros((size, 128), BF16)
            return 0

        lax.fori_loop(0, total, one, 0)

    pl.when(jnp.logical_not(has_up))(lambda: clear(0))
    pl.when(jnp.logical_not(has_down))(lambda: clear(1))

    for copy in small:
        copy.wait()
    mix = mixing[0]
    mix_up = jnp.where(has_up, mix, 0.0)
    mix_down = jnp.where(has_down, mix, 0.0)
    vert = [vertical[0, l] for l in range(levels - 1)]

    kind = raw[0]
    coeff = jnp.zeros((size, 128), F32)
    for index in range(regimes):
        coeff = coeff + jnp.where(kind == index, rates[0, index], 0.0)
    is_land = raw[1] == 1
    cx[1] = coeff
    land_scale[...] = jnp.where(is_land, 0.0, coeff)
    land_add[...] = jnp.where(is_land, coeff * land_add[...], 0.0)

    def coef_copies():
        up = pltpu.make_async_remote_copy(
            cx.at[1], cx.at[2], coef_send.at[0], coef_recv.at[1], device_id=(member, tile - 1), device_id_type=MESH
        )
        down = pltpu.make_async_remote_copy(
            cx.at[1], cx.at[0], coef_send.at[1], coef_recv.at[0], device_id=(member, tile + 1), device_id_type=MESH
        )
        return up, down

    def halo_copies(m):
        up = pltpu.make_async_remote_copy(
            hs.at[m, 0], hr.at[m, 1], halo_send.at[m, 0], halo_recv.at[m, 1],
            device_id=(member, tile - 1), device_id_type=MESH,
        )
        down = pltpu.make_async_remote_copy(
            hs.at[m, 1], hr.at[m, 0], halo_send.at[m, 1], halo_recv.at[m, 0],
            device_id=(member, tile + 1), device_id_type=MESH,
        )
        return up, down

    def start(copies):
        up, down = copies
        pl.when(has_up)(lambda: up.start())
        pl.when(has_down)(lambda: down.start())

    def wait_recv(copies):
        up, down = copies
        pl.when(has_up)(lambda: down.wait_recv())
        pl.when(has_down)(lambda: up.wait_recv())

    def wait_send(copies):
        up, down = copies
        pl.when(has_up)(lambda: up.wait_send())
        pl.when(has_down)(lambda: down.wait_send())

    def advance(cols, count, c, source):
        between = [vert[l] * (cols[l + 1] - cols[l]) for l in range(min(count, levels - 1))]
        new = [cols[0] + between[0] + (source - c * cols[0])]
        for l in range(1, count):
            if l < levels - 1:
                new.append(cols[l] + between[l] - between[l - 1])
            else:
                new.append(cols[l] - between[l - 1])
        return new

    top, bottom, from_up = strip_row == 0, strip_row == K - 1, strip_row >= 2

    def across(x):
        left = pltpu.roll(jnp.where(lane == 127, pltpu.roll(x, K, 0), x), 1, 1)
        right = pltpu.roll(jnp.where(lane == 0, pltpu.roll(x, size - K, 0), x), 127, 1)
        return left + right - 4.0 * x

    def turn(x, shift):
        return x if shift == 0 else pltpu.roll(x, shift % size, 0)

    def responses(m, window, source, ahead, send=True):
        slot = m % 4

        def one(p, _):
            rows = pl.ds(pl.multiple_of(p * 16, 16), 16)
            depth = 2 * K if ahead else K
            cols = [us[source, l, rows, :] for l in range(depth)]
            c = cx[1, rows, :]
            if ahead:
                for i in range(K):
                    cols = advance(cols, depth - 1 - i, c, q[window, i, rows, :])
            scale, add = land_scale[rows, :], land_add[rows, :]
            own[slot, 0, rows, :] = cols[0]
            for i in range(K - 1):
                cols = advance(cols, K - 1 - i, c, add + scale * force[K * m + i, rows, :])
                own[slot, i + 1, rows, :] = cols[0]
            return 0

        lax.fori_loop(0, size // 16, one, 0)

        def closed(x):
            above = jnp.where(top, 0.0, pltpu.roll(x, 1, 0))
            below = jnp.where(bottom, 0.0, pltpu.roll(x, size - 1, 0))
            return mix * (above + below + across(x))

        v0 = vert[0]
        gain = 1.0 - v0 - cx[1]
        ends = [own[slot, 0]]
        first = closed(ends[0])
        ends.append(own[slot, 1] + first)
        second = gain * first + closed(ends[1])
        ends.append(own[slot, 2] + second)
        ends.append(own[slot, 3] + gain * second + v0 * v0 * first + closed(ends[2]))
        to_up, to_down = ends[0], turn(ends[0], -3)
        for i in range(1, K):
            to_up = jnp.where(strip_row == i, turn(ends[i], i), to_up)
            to_down = jnp.where(strip_row == i, turn(ends[i], i - 3), to_down)
        hs[m, 0] = to_up.astype(BF16)
        hs[m, 1] = to_down.astype(BF16)
        if send:
            start(halo_copies(m))

    def simulate(m, window):
        slot = m % 4
        v0 = vert[0]
        gain = 1.0 - v0 - cx[1]
        edge_mix = jnp.where(from_up, mix_up, mix_down)
        edge_gain = 1.0 - v0 - jnp.where(from_up, cx[0], cx[2])
        wait_recv(halo_copies(m))
        up, down = hr[m, 0].astype(F32), hr[m, 1].astype(F32)

        def lateral(i, mid, edge):
            before, after = turn(up, -i), turn(down, 3 - i)
            if edge is not None:
                before, after = before + turn(edge, -3), after + turn(edge, 3)
            above = jnp.where(top, before, pltpu.roll(mid, 1, 0))
            below = jnp.where(bottom, after, pltpu.roll(mid, size - 1, 0))
            out = mix * (above + below + across(mid))
            q[window, i] = land_add[...] + land_scale[...] * force[K * m + i] + out
            return out

        def beyond(mid, edge):
            above = jnp.where(top, turn(mid, -3), pltpu.roll(edge, 1, 0))
            below = jnp.where(bottom, turn(mid, 3), pltpu.roll(edge, size - 1, 0))
            return edge_mix * (above + below + across(edge))

        mid = own[slot, 0]
        mid_1 = lateral(0, mid, None)
        edge_1 = edge_mix * jnp.where(top, turn(mid, -3), jnp.where(bottom, turn(mid, 3), 0.0))
        mid = own[slot, 1] + mid_1
        mid_2 = gain * mid_1 + lateral(1, mid, edge_1)
        edge_2 = edge_gain * edge_1 + beyond(mid, edge_1)
        mid = own[slot, 2] + mid_2
        mid_3 = gain * mid_2 + v0 * v0 * mid_1 + lateral(2, mid, edge_2)
        edge_3 = edge_gain * edge_2 + v0 * v0 * edge_1 + beyond(mid, edge_2)
        lateral(3, own[slot, 3] + mid_3, edge_3)

    def swap(x):
        r = lax.broadcasted_iota(jnp.int32, x.shape, 0) % 2
        high = lax.broadcasted_iota(jnp.int32, x.shape, 1) >= 64
        other = pltpu.roll(x, 64, 1)
        n = x.shape[0]
        moved = jnp.where(r == 1, pltpu.roll(other, 1, 0), pltpu.roll(other, n - 1, 0))
        return jnp.where((r == 1) == high, x, moved)

    def columns(m, window, source, depth, keep, trace=True):
        at = (m % 2) * K

        def one(p, _):
            rows = pl.ds(pl.multiple_of(p * 8, 8), 8)
            cols = [us[source, l, rows, :] for l in range(depth)]
            c = cx[1, rows, :]
            for i in range(K):
                cols = advance(cols, levels if depth == levels else depth - 1 - i, c, q[window, i, rows, :])
                if trace:
                    tr[i, rows, :] = cols[0]
            for l in range(keep):
                us[1 + window, l, rows, :] = cols[l]
            return 0

        lax.fori_loop(0, size // 8, one, 0)
        if trace:
            for i in range(K):
                sf[window, pl.ds(at + i, size, stride=8), :] = swap(tr[i])

    def trace_copy(g, o):
        return pltpu.make_async_remote_copy(
            snd.at[g, o], rcv.at[g, tile], trace_send.at[g], trace_recv.at[g],
            device_id=(1 - member, o), device_id_type=MESH,
        )

    def whole_trace(g):
        return pltpu.make_async_remote_copy(
            snd.at[g], rcv.at[g], trace_send.at[g], trace_recv.at[g], device_id=(1 - member, tile), device_id_type=MESH
        )

    def send_trace(g, window):
        def pack(j, _):
            for h in range(2):
                low = sf[window, pl.ds(pl.multiple_of((j * 4 + h) * 8, 8), 8), :]
                high = sf[window, pl.ds(pl.multiple_of((j * 4 + 2 + h) * 8, 8), 8), :]
                snd[g, 2 * j + h] = jnp.concatenate([low, high], axis=0).astype(BF16)
            return 0

        lax.fori_loop(0, tiles // 2, pack, 0, unroll=4)

        def send(k, _):
            trace_copy(g, lax.rem(tile + k, tiles)).start()
            return 0

        lax.fori_loop(0, tiles, send, 0, unroll=4)

    def product(g, begin, count):
        def one(j, _):
            for h in range(2):
                a = 2 * j + h
                block = rcv[g, a]
                cells = jnp.concatenate([block[:8], block[8:]], axis=1)
                out = lax.dot_general(cells, wts[a], (((1,), (1,)), ((), ())), preferred_element_type=F32)
                gf[pl.ds(pl.multiple_of((j * 4 + h) * 8, 8), 8), :] = out[:, :128]
                gf[pl.ds(pl.multiple_of((j * 4 + 2 + h) * 8, 8), 8), :] = out[:, 128:]
            return 0

        lax.fori_loop(begin // 2, (begin + count) // 2, one, 0, unroll=UNROLL)

    def spread(g):
        def one(t, _):
            force[steps + g * CHUNK + t] = swap(gf[pl.ds(t, size, stride=8), :])
            return 0

        lax.fori_loop(0, CHUNK, one, 0)

    def put(g):
        part = g - (ITERS - 1) * chunks
        return pltpu.make_async_copy(
            force.at[pl.ds(steps + g * CHUNK, CHUNK)], forcing.at[pl.ds(part * CHUNK, CHUNK)], out_sem.at[part]
        )

    for copy in early:
        copy.wait()
    responses(0, 0, 0, False, False)
    pl.semaphore_wait(barrier, tiles + jnp.where(has_up, 1, 0) + jnp.where(has_down, 1, 0))
    start(halo_copies(0))
    start(coef_copies())
    for copy in late:
        copy.wait()
    load_weights.start()
    wait_recv(coef_copies())

    def group(s, _):
        def members(body):
            def one(window, _):
                within = s - LAG * window

                @pl.when(jnp.logical_and(within >= 0, within < macros))
                def _():
                    body(window, within, macros * window + within, jnp.where(within == 0, 0, 1 + window))

                return 0

            lax.fori_loop(0, ITERS, one, 0)

        def surface(window, within, m, source):
            simulate(m, window)

            @pl.when(within < macros - 1)
            def _():
                responses(m + 1, window, source, True)

        def depth(window, within, m, source):
            end = window == ITERS - 1
            full = jnp.logical_or(within < macros - 2, jnp.logical_and(end, within < macros - 1))

            @pl.when(full)
            def _():
                columns(m, window, source, levels, levels)

            @pl.when(jnp.logical_and(jnp.logical_not(end), within == macros - 2))
            def _():
                columns(m, window, source, 2 * K + 1, K + 1)

            @pl.when(within == macros - 1)
            def _():
                columns(m, window, source, K + 1, 0)

            @pl.when(lax.rem(m, 2) == 1)
            def _():
                send_trace(m // 2, window)

            @pl.when(m == total - 1)
            def _():
                columns(m, window, source, levels, levels, False)

        members(surface)
        members(depth)

        @pl.when(s == LAG - 1)
        def _():
            load_weights.wait()

        @pl.when(jnp.logical_and(s >= LAG - 1, jnp.logical_and(s != LAG + 1, s < LAG + 1 + last - 1)))
        def _():
            g = jnp.where(s <= LAG, s - (LAG - 1), s - LAG)
            whole_trace(g).wait_recv()
            product(g, 0, tiles)
            spread(g)

        @pl.when(s == LAG - 1)
        def _():
            responses(macros, 1, 0, False)

        return 0

    lax.fori_loop(0, slots, group, 0)

    put_final = pltpu.make_async_copy(us.at[ITERS], final, out_sem.at[chunks])
    put_final.start()
    put(last - 2).start()
    put(last - 1).start()
    whole_trace(last).wait_recv()
    product(last, 0, tiles)
    spread(last)
    put(last).start()

    wait_send(coef_copies())

    def drain(m, _):
        wait_send(halo_copies(m))
        return 0

    lax.fori_loop(0, total, drain, 0)

    def drain_trace(g, _):
        whole_trace(g).wait_send()
        return 0

    lax.fori_loop(0, last + 1, drain_trace, 0)
    put_final.wait()
    for g in range(last - 2, last + 1):
        put(g).wait()


def to_tiles(x):
    n, rows, width = x.shape
    return x.reshape(n, rows, width // 128, 128).transpose(0, 2, 1, 3).reshape(n, rows * width // 128, 128)


def from_tiles(x, rows):
    n, size, _ = x.shape
    return x.reshape(n, size // rows, rows, 128).transpose(0, 2, 1, 3).reshape(n, rows, size // rows * 128)


def on_device(state, guess, regrid, regime, land, land_temp, exchange_rate, vertical, mixing):
    levels, rows, width = state.shape[1:]
    steps = guess.shape[1]
    tiles = lax.axis_size("tile")
    size = rows * width // 128
    cells = regrid.shape[-1]
    macros = ITERS * steps // K
    groups = ITERS * steps // CHUNK
    dims = (tiles, levels, steps, size, exchange_rate.shape[1])
    hbm = pl.BlockSpec(memory_space=pl.ANY)
    dma = pltpu.SemaphoreType.DMA
    final, forcing = pl.pallas_call(
        functools.partial(kernel, dims),
        out_shape=(
            jax.ShapeDtypeStruct((levels, size, 128), F32),
            jax.ShapeDtypeStruct((steps, size, 128), F32),
        ),
        in_specs=[hbm] * 8 + [pl.BlockSpec(memory_space=pltpu.SMEM)],
        out_specs=(hbm, hbm),
        scratch_shapes=[
            pltpu.SMEM(exchange_rate.shape, F32),
            pltpu.SMEM(vertical.shape, F32),
            pltpu.VMEM((1 + ITERS, levels, size, 128), F32),
            pltpu.VMEM(((ITERS + 1) * steps, size, 128), F32),
            pltpu.VMEM((tiles, cells, cells), BF16),
            pltpu.VMEM((3, size, 128), F32),
            pltpu.VMEM((2, size, 128), jnp.int32),
            pltpu.VMEM((size, 128), F32),
            pltpu.VMEM((size, 128), F32),
            pltpu.VMEM((4, K, size, 128), F32),
            pltpu.VMEM((macros, 2, size, 128), BF16),
            pltpu.VMEM((macros, 2, size, 128), BF16),
            pltpu.VMEM((ITERS, K, size, 128), F32),
            pltpu.VMEM((K, size, 128), F32),
            pltpu.VMEM((ITERS, 8 * size, 128), F32),
            pltpu.VMEM((groups, tiles, 16, 128), BF16),
            pltpu.VMEM((groups, tiles, 16, 128), BF16),
            pltpu.VMEM((8 * size, 128), F32),
            dma((10,)),
            dma((2,)),
            dma((2,)),
            dma((macros, 2)),
            dma((macros, 2)),
            dma((groups,)),
            dma((groups,)),
            dma((groups // ITERS + 1,)),
        ],
        compiler_params=pltpu.CompilerParams(
            collective_id=0, has_side_effects=True, vmem_limit_bytes=60 * 1024 * 1024
        ),
    )(
        to_tiles(state[0]),
        to_tiles(guess[0]),
        regrid[0, 0],
        to_tiles(regime)[0],
        to_tiles(land)[0],
        to_tiles(land_temp)[0],
        exchange_rate,
        vertical,
        mixing,
    )
    return from_tiles(final, rows)[None], from_tiles(forcing, rows)[None]


def solution(mesh):
    return jax.shard_map(
        on_device,
        mesh=mesh,
        in_specs=(
            P("mp", None, "tile", None),
            P("mp", None, "tile", None),
            P("mp", "tile", None, None, None),
            P("mp", "tile", None),
            P("mp", "tile", None),
            P("mp", "tile", None),
            P("mp", None),
            P("mp", None),
            P("mp"),
        ),
        out_specs=(P("mp", None, "tile", None), P("mp", None, "tile", None)),
        check_vma=False,
    )
```

```python
import functools

import jax
import jax.numpy as jnp
from jax import lax
from jax.experimental import pallas as pl
from jax.experimental.pallas import tpu as pltpu
from jax.sharding import PartitionSpec as P

MESH = pl.DeviceIdType.MESH
F32 = jnp.float32
BF16 = jnp.bfloat16
K = 4
CHUNK = 8
ITERS = 2
UNROLL = 8
LAG = 4


def kernel(
    dims,
    state, guess, regrid, regime, land, land_temp, rates_in, vertical_in, mixing,
    final, forcing,
    rates, vertical, us, force, wts, cx, raw, land_scale, land_add, own, hs, hr, q, tr, sf, snd, rcv, gf,
    in_sem, coef_send, coef_recv, halo_send, halo_recv, trace_send, trace_recv, out_sem,
):
    tiles, levels, steps, size, regimes = dims
    macros = steps // K
    chunks = steps // CHUNK
    total = ITERS * macros
    slots = macros + LAG * (ITERS - 1)
    last = ITERS * chunks - 1
    member = lax.axis_index("mp")
    tile = lax.axis_index("tile")
    has_up, has_down = tile > 0, tile < tiles - 1

    row = lax.broadcasted_iota(jnp.int32, (size, 128), 0)
    lane = lax.broadcasted_iota(jnp.int32, (size, 128), 1)
    strip_row = row % K

    small = [
        pltpu.make_async_copy(regime, raw.at[0], in_sem.at[0]),
        pltpu.make_async_copy(land, raw.at[1], in_sem.at[1]),
        pltpu.make_async_copy(land_temp, land_add, in_sem.at[2]),
        pltpu.make_async_copy(rates_in, rates, in_sem.at[8]),
        pltpu.make_async_copy(vertical_in, vertical, in_sem.at[9]),
    ]
    def load_state(begin, count, sem):
        part = pl.ds(begin, count)
        return pltpu.make_async_copy(state.at[part], us.at[0, part], in_sem.at[sem])

    def load_guess(begin, count, sem):
        part = pl.ds(begin, count)
        return pltpu.make_async_copy(guess.at[part], force.at[part], in_sem.at[sem])

    early = [load_state(0, K, 3), load_guess(0, K, 4)]
    late = [load_state(K, levels - K, 5), load_guess(K, steps - K, 6)]
    load_weights = pltpu.make_async_copy(regrid, wts, in_sem.at[7])
    for copy in small + early + late:
        copy.start()

    barrier = pltpu.get_barrier_semaphore()

    def greet(o, _):
        pl.semaphore_signal(barrier, inc=1, device_id=(1 - member, o), device_id_type=MESH)
        return 0

    lax.fori_loop(0, tiles, greet, 0, unroll=4)

    @pl.when(has_up)
    def _():
        pl.semaphore_signal(barrier, inc=1, device_id=(member, tile - 1), device_id_type=MESH)

    @pl.when(has_down)
    def _():
        pl.semaphore_signal(barrier, inc=1, device_id=(member, tile + 1), device_id_type=MESH)

    def clear(side):
        cx[2 * side] = jnp.zeros((size, 128), F32)

        def one(m, _):
            hr[m, side] = jnp.zeros((size, 128), BF16)
            return 0

        lax.fori_loop(0, total, one, 0)

    pl.when(jnp.logical_not(has_up))(lambda: clear(0))
    pl.when(jnp.logical_not(has_down))(lambda: clear(1))

    for copy in small:
        copy.wait()
    mix = mixing[0]
    mix_up = jnp.where(has_up, mix, 0.0)
    mix_down = jnp.where(has_down, mix, 0.0)
    vert = [vertical[0, l] for l in range(levels - 1)]

    kind = raw[0]
    coeff = jnp.zeros((size, 128), F32)
    for index in range(regimes):
        coeff = coeff + jnp.where(kind == index, rates[0, index], 0.0)
    is_land = raw[1] == 1
    cx[1] = coeff
    land_scale[...] = jnp.where(is_land, 0.0, coeff)
    land_add[...] = jnp.where(is_land, coeff * land_add[...], 0.0)

    def coef_copies():
        up = pltpu.make_async_remote_copy(
            cx.at[1], cx.at[2], coef_send.at[0], coef_recv.at[1], device_id=(member, tile - 1), device_id_type=MESH
        )
        down = pltpu.make_async_remote_copy(
            cx.at[1], cx.at[0], coef_send.at[1], coef_recv.at[0], device_id=(member, tile + 1), device_id_type=MESH
        )
        return up, down

    def halo_copies(m):
        up = pltpu.make_async_remote_copy(
            hs.at[m, 0], hr.at[m, 1], halo_send.at[m, 0], halo_recv.at[m, 1],
            device_id=(member, tile - 1), device_id_type=MESH,
        )
        down = pltpu.make_async_remote_copy(
            hs.at[m, 1], hr.at[m, 0], halo_send.at[m, 1], halo_recv.at[m, 0],
            device_id=(member, tile + 1), device_id_type=MESH,
        )
        return up, down

    def start(copies):
        up, down = copies
        pl.when(has_up)(lambda: up.start())
        pl.when(has_down)(lambda: down.start())

    def wait_recv(copies):
        up, down = copies
        pl.when(has_up)(lambda: down.wait_recv())
        pl.when(has_down)(lambda: up.wait_recv())

    def wait_send(copies):
        up, down = copies
        pl.when(has_up)(lambda: up.wait_send())
        pl.when(has_down)(lambda: down.wait_send())

    def advance(cols, count, c, source):
        between = [vert[l] * (cols[l + 1] - cols[l]) for l in range(min(count, levels - 1))]
        new = [cols[0] + between[0] + (source - c * cols[0])]
        for l in range(1, count):
            if l < levels - 1:
                new.append(cols[l] + between[l] - between[l - 1])
            else:
                new.append(cols[l] - between[l - 1])
        return new

    top, bottom, from_up = strip_row == 0, strip_row == K - 1, strip_row >= 2

    def across(x):
        left = pltpu.roll(jnp.where(lane == 127, pltpu.roll(x, K, 0), x), 1, 1)
        right = pltpu.roll(jnp.where(lane == 0, pltpu.roll(x, size - K, 0), x), 127, 1)
        return left + right - 4.0 * x

    def turn(x, shift):
        return x if shift == 0 else pltpu.roll(x, shift % size, 0)

    def responses(m, window, source, ahead, send=True):
        slot = m % 4

        def one(p, _):
            rows = pl.ds(pl.multiple_of(p * 16, 16), 16)
            depth = 2 * K if ahead else K
            cols = [us[source, l, rows, :] for l in range(depth)]
            c = cx[1, rows, :]
            if ahead:
                for i in range(K):
                    cols = advance(cols, depth - 1 - i, c, q[window, i, rows, :])
            scale, add = land_scale[rows, :], land_add[rows, :]
            own[slot, 0, rows, :] = cols[0]
            for i in range(K - 1):
                cols = advance(cols, K - 1 - i, c, add + scale * force[K * m + i, rows, :])
                own[slot, i + 1, rows, :] = cols[0]
            return 0

        lax.fori_loop(0, size // 16, one, 0, unroll=2)

        def closed(x):
            above = jnp.where(top, 0.0, pltpu.roll(x, 1, 0))
            below = jnp.where(bottom, 0.0, pltpu.roll(x, size - 1, 0))
            return mix * (above + below + across(x))

        v0 = vert[0]
        gain = 1.0 - v0 - cx[1]
        ends = [own[slot, 0]]
        first = closed(ends[0])
        own[slot, K] = first
        ends.append(own[slot, 1] + first)
        second = gain * first + closed(ends[1])
        ends.append(own[slot, 2] + second)
        ends.append(own[slot, 3] + gain * second + v0 * v0 * first + closed(ends[2]))
        to_up, to_down = ends[0], turn(ends[0], -3)
        for i in range(1, K):
            to_up = jnp.where(strip_row == i, turn(ends[i], i), to_up)
            to_down = jnp.where(strip_row == i, turn(ends[i], i - 3), to_down)
        hs[m, 0] = to_up.astype(BF16)
        hs[m, 1] = to_down.astype(BF16)
        if send:
            start(halo_copies(m))

    def simulate(m, window):
        slot = m % 4
        v0 = vert[0]
        gain = 1.0 - v0 - cx[1]
        edge_mix = jnp.where(from_up, mix_up, mix_down)
        edge_gain = 1.0 - v0 - jnp.where(from_up, cx[0], cx[2])
        mid = own[slot, 0]
        inside = jnp.where(top, turn(mid, -3), jnp.where(bottom, turn(mid, 3), 0.0))
        edge_1 = edge_mix * inside
        edge_ahead = (
            jnp.where(top, 0.0, pltpu.roll(edge_1, 1, 0))
            + jnp.where(bottom, 0.0, pltpu.roll(edge_1, size - 1, 0))
            + across(edge_1)
        )
        for i in range(K):
            q[window, i] = land_add[...] + land_scale[...] * force[K * m + i]
        wait_recv(halo_copies(m))
        up, down = hr[m, 0].astype(F32), hr[m, 1].astype(F32)

        def lateral(i, mid, edge):
            before, after = turn(up, -i) + turn(edge, -3), turn(down, 3 - i) + turn(edge, 3)
            above = jnp.where(top, before, pltpu.roll(mid, 1, 0))
            below = jnp.where(bottom, after, pltpu.roll(mid, size - 1, 0))
            out = mix * (above + below + across(mid))
            q[window, i] += out
            return out

        mid_1 = own[slot, K] + mix * jnp.where(top, up, jnp.where(bottom, turn(down, 3), 0.0))
        q[window, 0] += mid_1
        mid = own[slot, 1] + mid_1
        inside = jnp.where(top, turn(mid, -3), jnp.where(bottom, turn(mid, 3), 0.0))
        edge_2 = edge_gain * edge_1 + edge_mix * (edge_ahead + inside)
        mid_2 = gain * mid_1 + lateral(1, mid, edge_1)
        mid = own[slot, 2] + mid_2
        above = jnp.where(top, turn(mid, -3), pltpu.roll(edge_2, 1, 0))
        below = jnp.where(bottom, turn(mid, 3), pltpu.roll(edge_2, size - 1, 0))
        edge_3 = edge_gain * edge_2 + v0 * v0 * edge_1 + edge_mix * (above + below + across(edge_2))
        mid_3 = gain * mid_2 + v0 * v0 * mid_1 + lateral(2, mid, edge_2)
        lateral(3, own[slot, 3] + mid_3, edge_3)

    def swap(x):
        r = lax.broadcasted_iota(jnp.int32, x.shape, 0) % 2
        high = lax.broadcasted_iota(jnp.int32, x.shape, 1) >= 64
        other = pltpu.roll(x, 64, 1)
        n = x.shape[0]
        moved = jnp.where(r == 1, pltpu.roll(other, 1, 0), pltpu.roll(other, n - 1, 0))
        return jnp.where((r == 1) == high, x, moved)

    def columns(m, window, source, depth, keep, trace=True):
        at = (m % 2) * K

        def one(p, _):
            rows = pl.ds(pl.multiple_of(p * 8, 8), 8)
            cols = [us[source, l, rows, :] for l in range(depth)]
            c = cx[1, rows, :]
            for i in range(K):
                cols = advance(cols, levels if depth == levels else depth - 1 - i, c, q[window, i, rows, :])
                if trace:
                    tr[i, rows, :] = cols[0]
            for l in range(keep):
                us[1 + window, l, rows, :] = cols[l]
            return 0

        lax.fori_loop(0, size // 8, one, 0, unroll=2)
        if trace:
            for i in range(K):
                sf[window, pl.ds(at + i, size, stride=8), :] = swap(tr[i])

    def trace_copy(g, o):
        return pltpu.make_async_remote_copy(
            snd.at[g, o], rcv.at[g, tile], trace_send.at[g], trace_recv.at[g],
            device_id=(1 - member, o), device_id_type=MESH,
        )

    def whole_trace(g):
        return pltpu.make_async_remote_copy(
            snd.at[g], rcv.at[g], trace_send.at[g], trace_recv.at[g], device_id=(1 - member, tile), device_id_type=MESH
        )

    def send_trace(g, window):
        def pack(j, _):
            for h in range(2):
                low = sf[window, pl.ds(pl.multiple_of((j * 4 + h) * 8, 8), 8), :]
                high = sf[window, pl.ds(pl.multiple_of((j * 4 + 2 + h) * 8, 8), 8), :]
                snd[g, 2 * j + h] = jnp.concatenate([low, high], axis=0).astype(BF16)
            return 0

        lax.fori_loop(0, tiles // 2, pack, 0, unroll=4)

        def send(k, _):
            trace_copy(g, lax.rem(tile + k, tiles)).start()
            return 0

        lax.fori_loop(0, tiles, send, 0, unroll=4)

    def product(g, begin, count):
        def one(j, _):
            for h in range(2):
                a = 2 * j + h
                block = rcv[g, a]
                cells = jnp.concatenate([block[:8], block[8:]], axis=1)
                out = lax.dot_general(cells, wts[a], (((1,), (1,)), ((), ())), preferred_element_type=F32)
                gf[pl.ds(pl.multiple_of((j * 4 + h) * 8, 8), 8), :] = out[:, :128]
                gf[pl.ds(pl.multiple_of((j * 4 + 2 + h) * 8, 8), 8), :] = out[:, 128:]
            return 0

        lax.fori_loop(begin // 2, (begin + count) // 2, one, 0, unroll=UNROLL)

    def spread(g):
        def one(t, _):
            force[steps + g * CHUNK + t] = swap(gf[pl.ds(t, size, stride=8), :])
            return 0

        lax.fori_loop(0, CHUNK, one, 0)

    def put(g):
        part = g - (ITERS - 1) * chunks
        return pltpu.make_async_copy(
            force.at[pl.ds(steps + g * CHUNK, CHUNK)], forcing.at[pl.ds(part * CHUNK, CHUNK)], out_sem.at[part]
        )

    for copy in early:
        copy.wait()
    responses(0, 0, 0, False, False)
    pl.semaphore_wait(barrier, tiles + jnp.where(has_up, 1, 0) + jnp.where(has_down, 1, 0))
    start(halo_copies(0))
    start(coef_copies())
    for copy in late:
        copy.wait()
    load_weights.start()
    wait_recv(coef_copies())

    def group(s, _):
        def members(body):
            def one(window, _):
                within = s - LAG * window

                @pl.when(jnp.logical_and(within >= 0, within < macros))
                def _():
                    body(window, within, macros * window + within, jnp.where(within == 0, 0, 1 + window))

                return 0

            lax.fori_loop(0, ITERS, one, 0)

        def surface(window, within, m, source):
            simulate(m, window)

            @pl.when(within < macros - 1)
            def _():
                responses(m + 1, window, source, True)

        def depth(window, within, m, source):
            end = window == ITERS - 1
            full = jnp.logical_or(within < macros - 2, jnp.logical_and(end, within < macros - 1))

            @pl.when(full)
            def _():
                columns(m, window, source, levels, levels)

            @pl.when(jnp.logical_and(jnp.logical_not(end), within == macros - 2))
            def _():
                columns(m, window, source, 2 * K + 1, K + 1)

            @pl.when(within == macros - 1)
            def _():
                columns(m, window, source, K + 1, 0)

            @pl.when(lax.rem(m, 2) == 1)
            def _():
                send_trace(m // 2, window)

            @pl.when(m == total - 1)
            def _():
                columns(m, window, source, levels, levels, False)

        members(surface)
        members(depth)

        @pl.when(s == LAG - 1)
        def _():
            load_weights.wait()

        @pl.when(jnp.logical_or(s == LAG - 1, jnp.logical_and(s >= LAG, lax.rem(s - LAG, 2) == 0)))
        def _():
            g = jnp.where(s < LAG, 0, (s - LAG) // 2 + 1)
            whole_trace(g).wait_recv()
            product(g, 0, tiles)
            spread(g)

        @pl.when(s == LAG - 1)
        def _():
            responses(macros, 1, 0, False)

        return 0

    lax.fori_loop(0, slots, group, 0)

    put_final = pltpu.make_async_copy(us.at[ITERS], final, out_sem.at[chunks])
    put_final.start()
    put(last - 2).start()
    whole_trace(last - 1).wait_recv()
    product(last - 1, 0, tiles)
    spread(last - 1)
    put(last - 1).start()
    whole_trace(last).wait_recv()
    product(last, 0, tiles)
    spread(last)
    put(last).start()

    wait_send(coef_copies())

    def drain(m, _):
        wait_send(halo_copies(m))
        return 0

    lax.fori_loop(0, total, drain, 0)

    def drain_trace(g, _):
        whole_trace(g).wait_send()
        return 0

    lax.fori_loop(0, last + 1, drain_trace, 0)
    put_final.wait()
    for g in range(last - 2, last + 1):
        put(g).wait()


def to_tiles(x):
    n, rows, width = x.shape
    return x.reshape(n, rows, width // 128, 128).transpose(0, 2, 1, 3).reshape(n, rows * width // 128, 128)


def from_tiles(x, rows):
    n, size, _ = x.shape
    return x.reshape(n, size // rows, rows, 128).transpose(0, 2, 1, 3).reshape(n, rows, size // rows * 128)


def on_device(state, guess, regrid, regime, land, land_temp, exchange_rate, vertical, mixing):
    levels, rows, width = state.shape[1:]
    steps = guess.shape[1]
    tiles = lax.axis_size("tile")
    size = rows * width // 128
    cells = regrid.shape[-1]
    macros = ITERS * steps // K
    groups = ITERS * steps // CHUNK
    dims = (tiles, levels, steps, size, exchange_rate.shape[1])
    hbm = pl.BlockSpec(memory_space=pl.ANY)
    dma = pltpu.SemaphoreType.DMA
    final, forcing = pl.pallas_call(
        functools.partial(kernel, dims),
        out_shape=(
            jax.ShapeDtypeStruct((levels, size, 128), F32),
            jax.ShapeDtypeStruct((steps, size, 128), F32),
        ),
        in_specs=[hbm] * 8 + [pl.BlockSpec(memory_space=pltpu.SMEM)],
        out_specs=(hbm, hbm),
        scratch_shapes=[
            pltpu.SMEM(exchange_rate.shape, F32),
            pltpu.SMEM(vertical.shape, F32),
            pltpu.VMEM((1 + ITERS, levels, size, 128), F32),
            pltpu.VMEM(((ITERS + 1) * steps, size, 128), F32),
            pltpu.VMEM((tiles, cells, cells), BF16),
            pltpu.VMEM((3, size, 128), F32),
            pltpu.VMEM((2, size, 128), jnp.int32),
            pltpu.VMEM((size, 128), F32),
            pltpu.VMEM((size, 128), F32),
            pltpu.VMEM((4, K + 1, size, 128), F32),
            pltpu.VMEM((macros, 2, size, 128), BF16),
            pltpu.VMEM((macros, 2, size, 128), BF16),
            pltpu.VMEM((ITERS, K, size, 128), F32),
            pltpu.VMEM((K, size, 128), F32),
            pltpu.VMEM((ITERS, 8 * size, 128), F32),
            pltpu.VMEM((groups, tiles, 16, 128), BF16),
            pltpu.VMEM((groups, tiles, 16, 128), BF16),
            pltpu.VMEM((8 * size, 128), F32),
            dma((10,)),
            dma((2,)),
            dma((2,)),
            dma((macros, 2)),
            dma((macros, 2)),
            dma((groups,)),
            dma((groups,)),
            dma((groups // ITERS + 1,)),
        ],
        compiler_params=pltpu.CompilerParams(
            collective_id=0, has_side_effects=True, vmem_limit_bytes=60 * 1024 * 1024
        ),
    )(
        to_tiles(state[0]),
        to_tiles(guess[0]),
        regrid[0, 0],
        to_tiles(regime)[0],
        to_tiles(land)[0],
        to_tiles(land_temp)[0],
        exchange_rate,
        vertical,
        mixing,
    )
    return from_tiles(final, rows)[None], from_tiles(forcing, rows)[None]


def solution(mesh):
    return jax.shard_map(
        on_device,
        mesh=mesh,
        in_specs=(
            P("mp", None, "tile", None),
            P("mp", None, "tile", None),
            P("mp", "tile", None, None, None),
            P("mp", "tile", None),
            P("mp", "tile", None),
            P("mp", "tile", None),
            P("mp", None),
            P("mp", None),
            P("mp"),
        ),
        out_specs=(P("mp", None, "tile", None), P("mp", None, "tile", None)),
        check_vma=False,
    )
```

```python
import functools

import jax
import jax.numpy as jnp
from jax import lax
from jax.experimental import pallas as pl
from jax.experimental.pallas import tpu as pltpu
from jax.sharding import PartitionSpec as P

MESH = pl.DeviceIdType.MESH
F32 = jnp.float32
BF16 = jnp.bfloat16
K = 4
CHUNK = 8
ITERS = 2
UNROLL = 8
LAG = 4


def kernel(
    dims,
    state, guess, regrid, regime, land, land_temp, rates_in, vertical_in, mixing,
    final, forcing,
    rates, vertical, us, force, wts, cx, raw, land_scale, land_add, own, hs, hr, q, tr, sf, snd, rcv, gf,
    in_sem, coef_send, coef_recv, halo_send, halo_recv, trace_send, trace_recv, out_sem,
):
    tiles, levels, steps, size, regimes = dims
    macros = steps // K
    chunks = steps // CHUNK
    total = ITERS * macros
    slots = macros + LAG * (ITERS - 1)
    last = ITERS * chunks - 1
    member = lax.axis_index("mp")
    tile = lax.axis_index("tile")
    has_up, has_down = tile > 0, tile < tiles - 1

    row = lax.broadcasted_iota(jnp.int32, (size, 128), 0)
    lane = lax.broadcasted_iota(jnp.int32, (size, 128), 1)
    strip_row = row % K

    small = [
        pltpu.make_async_copy(regime, raw.at[0], in_sem.at[0]),
        pltpu.make_async_copy(land, raw.at[1], in_sem.at[1]),
        pltpu.make_async_copy(land_temp, land_add, in_sem.at[2]),
        pltpu.make_async_copy(rates_in, rates, in_sem.at[8]),
        pltpu.make_async_copy(vertical_in, vertical, in_sem.at[9]),
    ]
    def load_state(begin, count, sem):
        part = pl.ds(begin, count)
        return pltpu.make_async_copy(state.at[part], us.at[0, part], in_sem.at[sem])

    def load_guess(begin, count, sem):
        part = pl.ds(begin, count)
        return pltpu.make_async_copy(guess.at[part], force.at[part], in_sem.at[sem])

    early = [load_state(0, K, 3), load_guess(0, K, 4)]
    late = [load_state(K, levels - K, 5), load_guess(K, steps - K, 6)]
    load_weights = pltpu.make_async_copy(regrid, wts, in_sem.at[7])
    for copy in small + early + late:
        copy.start()

    barrier = pltpu.get_barrier_semaphore()

    def greet(k, _):
        o = lax.rem(tile + tiles // 2 + k, tiles)
        pl.semaphore_signal(barrier, inc=1, device_id=(1 - member, o), device_id_type=MESH)
        return 0

    lax.fori_loop(0, tiles, greet, 0, unroll=4)

    @pl.when(has_up)
    def _():
        pl.semaphore_signal(barrier, inc=1, device_id=(member, tile - 1), device_id_type=MESH)

    @pl.when(has_down)
    def _():
        pl.semaphore_signal(barrier, inc=1, device_id=(member, tile + 1), device_id_type=MESH)

    def clear(side):
        cx[2 * side] = jnp.zeros((size, 128), F32)

        def one(m, _):
            hr[m, side] = jnp.zeros((size, 128), BF16)
            return 0

        lax.fori_loop(0, total, one, 0)

    pl.when(jnp.logical_not(has_up))(lambda: clear(0))
    pl.when(jnp.logical_not(has_down))(lambda: clear(1))

    for copy in small:
        copy.wait()
    mix = mixing[0]
    mix_up = jnp.where(has_up, mix, 0.0)
    mix_down = jnp.where(has_down, mix, 0.0)
    vert = [vertical[0, l] for l in range(levels - 1)]

    kind = raw[0]
    coeff = jnp.zeros((size, 128), F32)
    for index in range(regimes):
        coeff = coeff + jnp.where(kind == index, rates[0, index], 0.0)
    is_land = raw[1] == 1
    cx[1] = coeff
    land_scale[...] = jnp.where(is_land, 0.0, coeff)
    land_add[...] = jnp.where(is_land, coeff * land_add[...], 0.0)

    def coef_copies():
        up = pltpu.make_async_remote_copy(
            cx.at[1], cx.at[2], coef_send.at[0], coef_recv.at[1], device_id=(member, tile - 1), device_id_type=MESH
        )
        down = pltpu.make_async_remote_copy(
            cx.at[1], cx.at[0], coef_send.at[1], coef_recv.at[0], device_id=(member, tile + 1), device_id_type=MESH
        )
        return up, down

    def halo_copies(m):
        up = pltpu.make_async_remote_copy(
            hs.at[m, 0], hr.at[m, 1], halo_send.at[m, 0], halo_recv.at[m, 1],
            device_id=(member, tile - 1), device_id_type=MESH,
        )
        down = pltpu.make_async_remote_copy(
            hs.at[m, 1], hr.at[m, 0], halo_send.at[m, 1], halo_recv.at[m, 0],
            device_id=(member, tile + 1), device_id_type=MESH,
        )
        return up, down

    def start(copies):
        up, down = copies
        pl.when(has_up)(lambda: up.start())
        pl.when(has_down)(lambda: down.start())

    def wait_recv(copies):
        up, down = copies
        pl.when(has_up)(lambda: down.wait_recv())
        pl.when(has_down)(lambda: up.wait_recv())

    def wait_send(copies):
        up, down = copies
        pl.when(has_up)(lambda: up.wait_send())
        pl.when(has_down)(lambda: down.wait_send())

    def advance(cols, count, c, source):
        between = [vert[l] * (cols[l + 1] - cols[l]) for l in range(min(count, levels - 1))]
        new = [cols[0] + between[0] + (source - c * cols[0])]
        for l in range(1, count):
            if l < levels - 1:
                new.append(cols[l] + between[l] - between[l - 1])
            else:
                new.append(cols[l] - between[l - 1])
        return new

    top, bottom, from_up = strip_row == 0, strip_row == K - 1, strip_row >= 2

    def across(x):
        left = pltpu.roll(jnp.where(lane == 127, pltpu.roll(x, K, 0), x), 1, 1)
        right = pltpu.roll(jnp.where(lane == 0, pltpu.roll(x, size - K, 0), x), 127, 1)
        return left + right - 4.0 * x

    def turn(x, shift):
        return x if shift == 0 else pltpu.roll(x, shift % size, 0)

    def responses(m, window, source, ahead, send=True):
        slot = m % 4

        def one(p, _):
            rows = pl.ds(pl.multiple_of(p * 16, 16), 16)
            depth = 2 * K if ahead else K
            cols = [us[source, l, rows, :] for l in range(depth)]
            c = cx[1, rows, :]
            if ahead:
                for i in range(K):
                    cols = advance(cols, depth - 1 - i, c, q[window, i, rows, :])
            scale, add = land_scale[rows, :], land_add[rows, :]
            own[slot, 0, rows, :] = cols[0]
            for i in range(K - 1):
                cols = advance(cols, K - 1 - i, c, add + scale * force[K * m + i, rows, :])
                own[slot, i + 1, rows, :] = cols[0]
            return 0

        lax.fori_loop(0, size // 16, one, 0, unroll=2)

        def closed(x):
            above = jnp.where(top, 0.0, pltpu.roll(x, 1, 0))
            below = jnp.where(bottom, 0.0, pltpu.roll(x, size - 1, 0))
            return mix * (above + below + across(x))

        v0 = vert[0]
        gain = 1.0 - v0 - cx[1]
        ends = [own[slot, 0]]
        first = closed(ends[0])
        own[slot, K] = first
        ends.append(own[slot, 1] + first)
        second = gain * first + closed(ends[1])
        ends.append(own[slot, 2] + second)
        ends.append(own[slot, 3] + gain * second + v0 * v0 * first + closed(ends[2]))
        to_up, to_down = ends[0], turn(ends[0], -3)
        for i in range(1, K):
            to_up = jnp.where(strip_row == i, turn(ends[i], i), to_up)
            to_down = jnp.where(strip_row == i, turn(ends[i], i - 3), to_down)
        hs[m, 0] = to_up.astype(BF16)
        hs[m, 1] = to_down.astype(BF16)
        if send:
            start(halo_copies(m))

    def simulate(m, window):
        slot = m % 4
        v0 = vert[0]
        gain = 1.0 - v0 - cx[1]
        edge_mix = jnp.where(from_up, mix_up, mix_down)
        edge_gain = 1.0 - v0 - jnp.where(from_up, cx[0], cx[2])
        mid = own[slot, 0]
        inside = jnp.where(top, turn(mid, -3), jnp.where(bottom, turn(mid, 3), 0.0))
        edge_1 = edge_mix * inside
        edge_ahead = (
            jnp.where(top, 0.0, pltpu.roll(edge_1, 1, 0))
            + jnp.where(bottom, 0.0, pltpu.roll(edge_1, size - 1, 0))
            + across(edge_1)
        )
        for i in range(K):
            q[window, i] = land_add[...] + land_scale[...] * force[K * m + i]
        wait_recv(halo_copies(m))
        up, down = hr[m, 0].astype(F32), hr[m, 1].astype(F32)

        def lateral(i, mid, edge):
            before, after = turn(up, -i) + turn(edge, -3), turn(down, 3 - i) + turn(edge, 3)
            above = jnp.where(top, before, pltpu.roll(mid, 1, 0))
            below = jnp.where(bottom, after, pltpu.roll(mid, size - 1, 0))
            out = mix * (above + below + across(mid))
            q[window, i] += out
            return out

        mid_1 = own[slot, K] + mix * jnp.where(top, up, jnp.where(bottom, turn(down, 3), 0.0))
        q[window, 0] += mid_1
        mid = own[slot, 1] + mid_1
        inside = jnp.where(top, turn(mid, -3), jnp.where(bottom, turn(mid, 3), 0.0))
        edge_2 = edge_gain * edge_1 + edge_mix * (edge_ahead + inside)
        mid_2 = gain * mid_1 + lateral(1, mid, edge_1)
        mid = own[slot, 2] + mid_2
        above = jnp.where(top, turn(mid, -3), pltpu.roll(edge_2, 1, 0))
        below = jnp.where(bottom, turn(mid, 3), pltpu.roll(edge_2, size - 1, 0))
        edge_3 = edge_gain * edge_2 + v0 * v0 * edge_1 + edge_mix * (above + below + across(edge_2))
        mid_3 = gain * mid_2 + v0 * v0 * mid_1 + lateral(2, mid, edge_2)
        lateral(3, own[slot, 3] + mid_3, edge_3)

    def swap(x):
        r = lax.broadcasted_iota(jnp.int32, x.shape, 0) % 2
        high = lax.broadcasted_iota(jnp.int32, x.shape, 1) >= 64
        other = pltpu.roll(x, 64, 1)
        n = x.shape[0]
        moved = jnp.where(r == 1, pltpu.roll(other, 1, 0), pltpu.roll(other, n - 1, 0))
        return jnp.where((r == 1) == high, x, moved)

    def columns(m, window, source, depth, keep, trace=True):
        at = (m % 2) * K

        def one(p, _):
            rows = pl.ds(pl.multiple_of(p * 8, 8), 8)
            cols = [us[source, l, rows, :] for l in range(depth)]
            c = cx[1, rows, :]
            for i in range(K):
                cols = advance(cols, levels if depth == levels else depth - 1 - i, c, q[window, i, rows, :])
                if trace:
                    tr[i, rows, :] = cols[0]
            for l in range(keep):
                us[1 + window, l, rows, :] = cols[l]
            return 0

        lax.fori_loop(0, size // 8, one, 0, unroll=2)
        if trace:
            for i in range(K):
                sf[window, pl.ds(at + i, size, stride=8), :] = swap(tr[i])

    def trace_copy(g, o):
        return pltpu.make_async_remote_copy(
            snd.at[g, o], rcv.at[g, tile], trace_send.at[g], trace_recv.at[g],
            device_id=(1 - member, o), device_id_type=MESH,
        )

    def whole_trace(g):
        return pltpu.make_async_remote_copy(
            snd.at[g], rcv.at[g], trace_send.at[g], trace_recv.at[g], device_id=(1 - member, tile), device_id_type=MESH
        )

    def send_trace(g, window):
        def pack(j, _):
            for h in range(2):
                low = sf[window, pl.ds(pl.multiple_of((j * 4 + h) * 8, 8), 8), :]
                high = sf[window, pl.ds(pl.multiple_of((j * 4 + 2 + h) * 8, 8), 8), :]
                snd[g, 2 * j + h] = jnp.concatenate([low, high], axis=0).astype(BF16)
            return 0

        lax.fori_loop(0, tiles // 2, pack, 0, unroll=4)

        def send(k, _):
            trace_copy(g, lax.rem(tile + tiles // 2 + k, tiles)).start()
            return 0

        lax.fori_loop(0, tiles, send, 0, unroll=4)

    def product(g, begin, count):
        def one(j, _):
            for h in range(2):
                a = 2 * j + h
                block = rcv[g, a]
                cells = jnp.concatenate([block[:8], block[8:]], axis=1)
                out = lax.dot_general(cells, wts[a], (((1,), (1,)), ((), ())), preferred_element_type=F32)
                gf[pl.ds(pl.multiple_of((j * 4 + h) * 8, 8), 8), :] = out[:, :128]
                gf[pl.ds(pl.multiple_of((j * 4 + 2 + h) * 8, 8), 8), :] = out[:, 128:]
            return 0

        lax.fori_loop(begin // 2, (begin + count) // 2, one, 0, unroll=UNROLL)

    def spread(g):
        def one(t, _):
            force[steps + g * CHUNK + t] = swap(gf[pl.ds(t, size, stride=8), :])
            return 0

        lax.fori_loop(0, CHUNK, one, 0)

    def put(g):
        part = g - (ITERS - 1) * chunks
        return pltpu.make_async_copy(
            force.at[pl.ds(steps + g * CHUNK, CHUNK)], forcing.at[pl.ds(part * CHUNK, CHUNK)], out_sem.at[part]
        )

    for copy in early:
        copy.wait()
    responses(0, 0, 0, False, False)
    pl.semaphore_wait(barrier, tiles + jnp.where(has_up, 1, 0) + jnp.where(has_down, 1, 0))
    start(halo_copies(0))
    start(coef_copies())
    for copy in late:
        copy.wait()
    load_weights.start()
    wait_recv(coef_copies())

    def group(s, _):
        def members(body):
            def one(window, _):
                within = s - LAG * window

                @pl.when(jnp.logical_and(within >= 0, within < macros))
                def _():
                    body(window, within, macros * window + within, jnp.where(within == 0, 0, 1 + window))

                return 0

            lax.fori_loop(0, ITERS, one, 0)

        def surface(window, within, m, source):
            simulate(m, window)

            @pl.when(within < macros - 1)
            def _():
                responses(m + 1, window, source, True)

        def depth(window, within, m, source):
            end = window == ITERS - 1
            full = jnp.logical_or(within < macros - 2, jnp.logical_and(end, within < macros - 1))

            @pl.when(full)
            def _():
                columns(m, window, source, levels, levels)

            @pl.when(jnp.logical_and(jnp.logical_not(end), within == macros - 2))
            def _():
                columns(m, window, source, 2 * K + 1, K + 1)

            @pl.when(within == macros - 1)
            def _():
                columns(m, window, source, K + 1, 0)

            @pl.when(lax.rem(m, 2) == 1)
            def _():
                send_trace(m // 2, window)

            @pl.when(m == total - 1)
            def _():
                columns(m, window, source, levels, levels, False)

        members(surface)
        members(depth)

        @pl.when(s == LAG - 1)
        def _():
            load_weights.wait()

        @pl.when(jnp.logical_or(s == LAG - 1, jnp.logical_and(s >= LAG, lax.rem(s - LAG, 2) == 0)))
        def _():
            g = jnp.where(s < LAG, 0, (s - LAG) // 2 + 1)
            whole_trace(g).wait_recv()
            product(g, 0, tiles)
            spread(g)

        @pl.when(s == LAG - 1)
        def _():
            responses(macros, 1, 0, False)

        return 0

    lax.fori_loop(0, slots, group, 0)

    put_final = pltpu.make_async_copy(us.at[ITERS], final, out_sem.at[chunks])
    put_final.start()
    put(last - 2).start()
    whole_trace(last - 1).wait_recv()
    product(last - 1, 0, tiles)
    spread(last - 1)
    put(last - 1).start()
    whole_trace(last).wait_recv()
    product(last, 0, tiles)
    spread(last)
    put(last).start()

    wait_send(coef_copies())

    def drain(m, _):
        wait_send(halo_copies(m))
        return 0

    lax.fori_loop(0, total, drain, 0)

    def drain_trace(g, _):
        whole_trace(g).wait_send()
        return 0

    lax.fori_loop(0, last + 1, drain_trace, 0)
    put_final.wait()
    for g in range(last - 2, last + 1):
        put(g).wait()


def to_tiles(x):
    n, rows, width = x.shape
    return x.reshape(n, rows, width // 128, 128).transpose(0, 2, 1, 3).reshape(n, rows * width // 128, 128)


def from_tiles(x, rows):
    n, size, _ = x.shape
    return x.reshape(n, size // rows, rows, 128).transpose(0, 2, 1, 3).reshape(n, rows, size // rows * 128)


def on_device(state, guess, regrid, regime, land, land_temp, exchange_rate, vertical, mixing):
    levels, rows, width = state.shape[1:]
    steps = guess.shape[1]
    tiles = lax.axis_size("tile")
    size = rows * width // 128
    cells = regrid.shape[-1]
    macros = ITERS * steps // K
    groups = ITERS * steps // CHUNK
    dims = (tiles, levels, steps, size, exchange_rate.shape[1])
    hbm = pl.BlockSpec(memory_space=pl.ANY)
    dma = pltpu.SemaphoreType.DMA
    final, forcing = pl.pallas_call(
        functools.partial(kernel, dims),
        out_shape=(
            jax.ShapeDtypeStruct((levels, size, 128), F32),
            jax.ShapeDtypeStruct((steps, size, 128), F32),
        ),
        in_specs=[hbm] * 8 + [pl.BlockSpec(memory_space=pltpu.SMEM)],
        out_specs=(hbm, hbm),
        scratch_shapes=[
            pltpu.SMEM(exchange_rate.shape, F32),
            pltpu.SMEM(vertical.shape, F32),
            pltpu.VMEM((1 + ITERS, levels, size, 128), F32),
            pltpu.VMEM(((ITERS + 1) * steps, size, 128), F32),
            pltpu.VMEM((tiles, cells, cells), BF16),
            pltpu.VMEM((3, size, 128), F32),
            pltpu.VMEM((2, size, 128), jnp.int32),
            pltpu.VMEM((size, 128), F32),
            pltpu.VMEM((size, 128), F32),
            pltpu.VMEM((4, K + 1, size, 128), F32),
            pltpu.VMEM((macros, 2, size, 128), BF16),
            pltpu.VMEM((macros, 2, size, 128), BF16),
            pltpu.VMEM((ITERS, K, size, 128), F32),
            pltpu.VMEM((K, size, 128), F32),
            pltpu.VMEM((ITERS, 8 * size, 128), F32),
            pltpu.VMEM((groups, tiles, 16, 128), BF16),
            pltpu.VMEM((groups, tiles, 16, 128), BF16),
            pltpu.VMEM((8 * size, 128), F32),
            dma((10,)),
            dma((2,)),
            dma((2,)),
            dma((macros, 2)),
            dma((macros, 2)),
            dma((groups,)),
            dma((groups,)),
            dma((groups // ITERS + 1,)),
        ],
        compiler_params=pltpu.CompilerParams(
            collective_id=0, has_side_effects=True, vmem_limit_bytes=60 * 1024 * 1024
        ),
    )(
        to_tiles(state[0]),
        to_tiles(guess[0]),
        regrid[0, 0],
        to_tiles(regime)[0],
        to_tiles(land)[0],
        to_tiles(land_temp)[0],
        exchange_rate,
        vertical,
        mixing,
    )
    return from_tiles(final, rows)[None], from_tiles(forcing, rows)[None]


def solution(mesh):
    return jax.shard_map(
        on_device,
        mesh=mesh,
        in_specs=(
            P("mp", None, "tile", None),
            P("mp", None, "tile", None),
            P("mp", "tile", None, None, None),
            P("mp", "tile", None),
            P("mp", "tile", None),
            P("mp", "tile", None),
            P("mp", None),
            P("mp", None),
            P("mp"),
        ),
        out_specs=(P("mp", None, "tile", None), P("mp", None, "tile", None)),
        check_vma=False,
    )
```
